256 devices in a mesh: lat: 32 (over z, x), lev: 8 (over y, core).
Axes of the slice: x: 4, y: 4, z: 8, core: 2. Of those that a mesh axis runs over, the one named last changes fastest.
Arguments:
- pressure_thick: float32 [32, 768, 1152], P('lev', 'lat'), may hold values from 0.016 to 4.7
- potential_temp: float32 [32, 768, 1152], P('lev', 'lat'), may hold values from 0.5 to 3
- tracer: float32 [32, 768, 1152], P('lev', 'lat'), may hold values from 0 to 1
- east_courant: float32 [32, 768, 1152], P('lev', 'lat'), may hold values from -0.15 to 0.15
- north_courant: float32 [32, 768, 1152], P('lev', 'lat'), may hold values from -0.15 to 0.15
- polar_mask: int32 [768], P('lat'), may hold values from 0 to 1, as said below
- wave_cutoff: int32 [768], P('lat'), may hold values from 1 to 576, as said below
- level_weight: float32 [32], replicated, may hold values from 0.3 to 3
- target_surface: float32 [1], replicated, may hold values from 32 to 44.8
Outputs:
- remapped_thick: float32 [32, 768, 1152], P(None, 'lev', 'lat')
- remapped_temp: float32 [32, 768, 1152], P(None, 'lev', 'lat')
- remapped_tracer: float32 [32, 768, 1152], P(None, 'lev', 'lat')
The draws below stay inside these ranges and needn't reach their ends.
Inputs may be any that keep to these rules, and one draw needn't show every extreme that they name: `polar_mask`: 1 on the first and last P rows and 0 between, for one P from 96 to 153. `wave_cutoff`: rows with polar_mask 0 hold 576.
All inputs are finite; a program needn't handle non-finite values.
Results may differ from the reference program's by a relative error of at most 0.0003.
Values sent between devices are 32-bit elements; how exact they have to be, the bound alone decides.
A program may use at most 128 MiB of HBM per device.

```python
import math
import jax
import jax.numpy as jnp
from jax import lax

NLON = 1152
NLAT = 768
LEV = 32


def polar_caps(key):
    return jax.random.randint(jax.random.fold_in(key, 11), (), NLAT // 8, NLAT // 5 + 1)


def pole_distance():
    row_index = jnp.arange(NLAT, dtype=jnp.int32)
    return jnp.minimum(row_index, NLAT - 1 - row_index)


def draw_polar_mask(key, part):
    caps = polar_caps(key)
    return (pole_distance() < caps).astype(jnp.int32)


def draw_wave_cutoff(key, part):
    caps = polar_caps(key)
    distance = pole_distance()
    jitter = jax.random.randint(jax.random.fold_in(key, 13), (NLAT,), -2, 3)
    ramp = 1 + distance * (NLON // 2 - 1) // caps
    limited = jnp.clip(ramp + jitter, 1, NLON // 2)
    return jnp.where(distance < caps, limited, NLON // 2).astype(jnp.int32)


def draw_pressure_thick(key, part):
    height = jnp.arange(LEV, dtype=jnp.float32) / max(LEV - 1, 1)
    east_frac = jnp.arange(NLON, dtype=jnp.float32) / NLON
    north_frac = jnp.arange(NLAT, dtype=jnp.float32) / NLAT
    noise = jax.random.uniform(key, (LEV, NLAT, NLON), jnp.float32, 0.8, 1.2)
    lat_factor = 0.7 + 0.6 * north_frac
    base = 0.2 + 1.8 * height
    lon_factor = 0.5 + east_frac
    shape = base[:, None, None] * lat_factor[None, :, None] * lon_factor[None, None, :]
    return (shape * noise).astype(jnp.float32)


def levels(stream_key, extent, split, smallest, largest):
    factor_of = 1.0
    for dim, blocks in split:
        heights = jax.random.uniform(jax.random.fold_in(jax.random.fold_in(stream_key, 6), dim), (blocks,), jnp.float32, smallest / len(split), largest / len(split))
        factor_of = factor_of * jnp.repeat(jnp.exp(heights), extent[dim] // blocks).reshape((-1,) + (1,) * (len(extent) - 1 - dim))
    return factor_of


def setup_inputs(seed: int = 0) -> dict:
    streams_of = jax.random.split(jax.random.key(seed), 10)
    return {
        "pressure_thick": draw_pressure_thick(jax.random.fold_in(streams_of[9], 71), 0),
        "potential_temp": jnp.clip(0.5 + 2.5 * jax.random.uniform(streams_of[1], (LEV, NLAT, NLON), jnp.float32) ** levels(streams_of[1], (LEV, NLAT, NLON), ((0, 8), (1, 32)), -0.2, 0.2), 0.5, 3.0),
        "tracer": jnp.clip(1.0 * jax.random.uniform(streams_of[2], (LEV, NLAT, NLON), jnp.float32) ** levels(streams_of[2], (LEV, NLAT, NLON), ((0, 8), (1, 32)), -0.2, 0.2), 0.0, 1.0),
        "east_courant": jnp.clip(jax.random.uniform(streams_of[3], (LEV, NLAT, NLON), jnp.float32, -0.15, 0.15) * levels(streams_of[3], (LEV, NLAT, NLON), ((0, 8), (1, 32)), -0.4, 0.0), -0.15, 0.15),
        "north_courant": jnp.clip(jax.random.uniform(streams_of[4], (LEV, NLAT, NLON), jnp.float32, -0.15, 0.15) * levels(streams_of[4], (LEV, NLAT, NLON), ((0, 8), (1, 32)), -0.4, 0.0), -0.15, 0.15),
        "polar_mask": draw_polar_mask(jax.random.fold_in(streams_of[9], 71), 0),
        "wave_cutoff": draw_wave_cutoff(jax.random.fold_in(streams_of[9], 71), 0),
        "level_weight": jnp.clip(jnp.exp(jax.random.uniform(streams_of[7], (LEV,), jnp.float32, math.log(0.3), math.log(3.0))), 0.3, 3.0),
        "target_surface": jnp.clip(jax.random.uniform(streams_of[8], (1,), jnp.float32, 32.0, 44.8), 32.0, 44.8),
    }


def north_of(field):
    return jnp.pad(field, ((0, 0), (0, 1), (0, 0)))[:, 1:, :]


def south_of(field):
    return jnp.pad(field, ((0, 0), (1, 0), (0, 0)))[:, :-1, :]


def reference(pressure_thick, potential_temp, tracer, east_courant, north_courant, polar_mask, wave_cutoff, level_weight, target_surface):
    nlat = pressure_thick.shape[1]
    nlon = pressure_thick.shape[2]
    row_index = jnp.arange(nlat, dtype=jnp.float32)
    center_cos = jnp.sin((row_index + 0.5) * jnp.pi / nlat)
    face_cos = jnp.sin((row_index + 1.0) * jnp.pi / nlat)
    east_mass = east_courant * (pressure_thick + jnp.roll(pressure_thick, -1, axis=2)) * 0.5
    north_mass = north_courant * (pressure_thick + north_of(pressure_thick)) * 0.5 * face_cos[None, :, None]
    tendencies = []
    for scalar in (None, potential_temp, tracer):
        if scalar is None:
            east_part, north_part = east_mass, north_mass
        else:
            east_part = east_mass * (scalar + jnp.roll(scalar, -1, axis=2)) * 0.5
            north_part = north_mass * (scalar + north_of(scalar)) * 0.5
        diverge = (east_part - jnp.roll(east_part, 1, axis=2)) + (north_part - south_of(north_part)) / center_cos[None, :, None]
        tendencies.append(-diverge)
    wave = jnp.arange(nlon // 2 + 1, dtype=jnp.int32)
    keep = (polar_mask[:, None] > 0) & (wave[None, :] >= wave_cutoff[:, None])
    filtered = []
    for tendency in tendencies:
        spectrum = jnp.fft.rfft(tendency, axis=-1)
        high = jnp.fft.irfft(spectrum * keep[None, :, :], n=nlon, axis=-1)
        filtered.append(tendency - high.astype(tendency.dtype))
    new_thick = pressure_thick + filtered[0]
    new_temp = potential_temp + (filtered[1] - potential_temp * filtered[0]) / pressure_thick
    new_tracer = tracer + (filtered[2] - tracer * filtered[0]) / pressure_thick
    surface = jnp.sum(new_thick, axis=0)
    top_edge = jnp.cumsum(new_thick, axis=0) - new_thick
    share = level_weight / jnp.sum(level_weight)
    bound = surface[None] * jnp.cumsum(share)[:, None, None]

    def add_source(totals, source):
        thick_src, top_src, temp_src, tracer_src = source
        intersection = jnp.minimum(jnp.maximum(bound - top_src[None], 0.0), thick_src[None])
        return (totals[0] + temp_src[None] * intersection, totals[1] + tracer_src[None] * intersection), None

    zeros = jnp.zeros(bound.shape, jnp.float32)
    (cumul_temp, cumul_tracer), unused = lax.scan(add_source, (zeros, zeros), (new_thick, top_edge, new_temp, new_tracer))
    target_thick = surface[None] * share[:, None, None]
    remapped_temp = (cumul_temp - jnp.concatenate([zeros[:1], cumul_temp[:-1]], axis=0)) / target_thick
    remapped_tracer = (cumul_tracer - jnp.concatenate([zeros[:1], cumul_tracer[:-1]], axis=0)) / target_thick
    total = jnp.sum(new_thick * center_cos[None, :, None])
    mean_surface = total / (nlon * jnp.sum(center_cos))
    remapped_thick = target_thick * (target_surface[0] / mean_surface)
    return remapped_thick, remapped_temp, remapped_tracer
```

```python
import functools

import jax
import jax.numpy as jnp
import numpy as np
from jax import lax
from jax.experimental import pallas as pl
from jax.experimental.pallas import tpu as pltpu
from jax.sharding import PartitionSpec as P

MESH = pl.DeviceIdType.MESH
F32 = jnp.float32
BF16 = jnp.bfloat16

NLON, NLAT, LEV = 1152, 768, 32
ROWS = 24
LEVD = 4
NZ, NX, NY = 8, 4, 4
NLATD, NLEVD = 32, 8
RADIX, POINTS = 9, 128
SENT = 84
POLAR_BANDS = -(-(NLAT // 5) // ROWS)


def split_bf16(x):
    high = x.astype(BF16)
    return high, (x - high.astype(F32)).astype(BF16)


def tables():
    b = np.arange(POINTS)[:, None]
    full = np.zeros((4, 256, 256))
    for k1 in range(1, 5):
        angle = 2.0 * np.pi * ((b * (k1 + RADIX * np.arange(POINTS)[None, :])) % NLON) / NLON
        c, s = np.cos(angle), np.sin(angle)
        full[k1 - 1] = np.block([[c, -s], [s, c]])
    col = np.arange(POINTS)[None, :]
    wave = np.where(col <= 64, col, col - 64)
    angle = 2.0 * np.pi * ((b * wave) % POINTS) / POINTS
    real = np.where(col <= 64, np.cos(angle), np.sin(angle))

    def pair(x):
        high = x.astype(np.float32).astype(BF16)
        low = (x - high.astype(np.float64)).astype(np.float32).astype(BF16)
        return np.stack([np.asarray(high), np.asarray(low)])

    return pair(full), pair(real)


def dot3(xh, xl, th, tl, dims):
    dot = functools.partial(
        lax.dot_general, dimension_numbers=(dims, ((), ())), preferred_element_type=F32
    )
    return dot(xh, th) + dot(xl, th) + dot(xh, tl)


def lanes9(x):
    return jnp.concatenate([x] * RADIX, axis=1)


def dynamics_kernel(
    th_ref, te_ref, tr_ref, ec_ref, nc_ref, mask_ref, cut_ref, full_ref, real_ref,
    msg_ref, sum_ref,
    s_ref, up_ref, down_ref, from_south, from_north, uh_ref, ul_ref, z_ref, t_ref, send_sem, recv_sem,
):
    lat = lax.axis_index("lat")
    lev = lax.axis_index("lev")
    north = lax.rem(lat + 1, NLATD)
    south = lax.rem(lat + NLATD - 1, NLATD)

    barrier = pltpu.get_barrier_semaphore()
    for other in (north, south):
        pl.semaphore_signal(barrier, inc=1, device_id=(other, lev), device_id_type=MESH)
    fields = (th_ref, te_ref, tr_ref, nc_ref)
    for f in range(4):
        for l in range(LEVD):
            up_ref[pl.ds(4 * f + l, 1), :] = fields[f][l, ROWS - 1 : ROWS, :]
            if f < 3:
                down_ref[pl.ds(4 * f + l, 1), :] = fields[f][l, 0:1, :]
    pl.semaphore_wait(barrier, 2)
    to_north = pltpu.make_async_remote_copy(
        src_ref=up_ref, dst_ref=from_south, send_sem=send_sem.at[0], recv_sem=recv_sem.at[0],
        device_id=(north, lev), device_id_type=MESH,
    )
    to_south = pltpu.make_async_remote_copy(
        src_ref=down_ref, dst_ref=from_north, send_sem=send_sem.at[1], recv_sem=recv_sem.at[1],
        device_id=(south, lev), device_id_type=MESH,
    )
    to_north.start()
    to_south.start()

    first_row = lat * ROWS
    row = (first_row + lax.broadcasted_iota(jnp.int32, (ROWS, 128), 0)).astype(F32)
    center = lanes9(jnp.sin((row + 0.5) * np.float32(np.pi) / NLAT))
    face = lanes9(jnp.sin((row + 1.0) * np.float32(np.pi) / NLAT))
    face_below = face_below_row(first_row)
    inverse_center = 1.0 / center

    def shift_west(x):
        return pltpu.roll(x, NLON - 1, 1)

    def shift_east(x):
        return pltpu.roll(x, 1, 1)

    def east(l, carry):
        th, te, tr = th_ref[l], te_ref[l], tr_ref[l]
        mass = ec_ref[l] * (th + shift_west(th)) * 0.5
        temp = mass * (te + shift_west(te)) * 0.5
        trac = mass * (tr + shift_west(tr)) * 0.5
        s_ref[0, l] = shift_east(mass) - mass
        s_ref[1, l] = shift_east(temp) - temp
        s_ref[2, l] = shift_east(trac) - trac
        return carry

    lax.fori_loop(0, LEVD, east, 0)

    to_north.wait()
    to_south.wait()

    row_in = lax.broadcasted_iota(jnp.int32, (ROWS, NLON), 0)

    for l in range(LEVD):
        th, te, tr = th_ref[l], te_ref[l], tr_ref[l]

        def above(x, f):
            edge = from_north[4 * f + l : 4 * f + l + 1, :]
            edge = jnp.where(lat == NLATD - 1, 0.0, edge)
            return jnp.where(row_in == ROWS - 1, edge, pltpu.roll(x, ROWS - 1, 0))

        def south_row(f):
            return from_south[4 * f + l : 4 * f + l + 1, :]

        mass = nc_ref[l] * (th + above(th, 0)) * 0.5 * face
        temp = mass * (te + above(te, 1)) * 0.5
        trac = mass * (tr + above(tr, 2)) * 0.5
        mass_s = south_row(3) * (south_row(0) + th[0:1]) * 0.5 * face_below
        temp_s = mass_s * (south_row(1) + te[0:1]) * 0.5
        trac_s = mass_s * (south_row(2) + tr[0:1]) * 0.5
        for f, (flux, below) in enumerate(((mass, mass_s), (temp, temp_s), (trac, trac_s))):
            lower = jnp.where(row_in == 0, below, pltpu.roll(flux, 1, 0))
            s_ref[f, l] = s_ref[f, l] - (flux - lower) * inverse_center

    polar = jnp.logical_or(lat < POLAR_BANDS, lat >= NLATD - POLAR_BANDS)

    @pl.when(polar)
    def _():
        polar_filter(mask_ref, cut_ref, full_ref, real_ref, s_ref, uh_ref, ul_ref, z_ref)

    def update(l, total):
        th, te, tr = th_ref[l], te_ref[l], tr_ref[l]
        mass = s_ref[0, l]
        inverse = 1.0 / th
        new_th = th + mass
        s_ref[0, l] = new_th
        s_ref[1, l] = te + (s_ref[1, l] - te * mass) * inverse
        s_ref[2, l] = tr + (s_ref[2, l] - tr * mass) * inverse
        weighted = new_th * center
        for a in range(RADIX):
            part = weighted[:, 128 * a : 128 * a + 128]
            total = total + (part[0:8] + part[8:16] + part[16:24])
        return total

    total = lax.fori_loop(0, LEVD, update, jnp.zeros((8, 128), F32))
    sum_ref[...] = jnp.sum(total, axis=0, keepdims=True)

    flat = s_ref.reshape(3 * LEVD * ROWS, NLON)
    for a in range(RADIX):
        at = pl.ds(128 * a, 128)
        one = jnp.concatenate([flat[0:120, at], flat[264:272, at]], axis=0)
        two = jnp.concatenate([flat[120:240, at], flat[272:280, at]], axis=0)
        last = jnp.concatenate([flat[240:264, at], flat[280:288, at]], axis=0)
        t_ref[0, at, :] = one.T
        t_ref[1, at, :] = two.T
        t_ref[2, at, :] = jnp.concatenate([last] * 4, axis=0).T

    sub = lax.broadcasted_iota(jnp.int32, (8, 128), 0)
    lane = lax.broadcasted_iota(jnp.int32, (8, 128), 1)

    def pack(p, carry):
        base = 72 * p

        def tile(q, j, n=1):
            return t_ref[q, pl.ds(pl.multiple_of(base + 8 * j, 8), 8 * n), :]

        def fours(u):
            return jnp.where(
                lane < 64, jnp.where(lane < 32, u[0], u[1]), jnp.where(lane < 96, u[2], u[3])
            )

        for q in range(2):
            msg_ref[2 * p, 32 * q : 32 * q + 32, :] = tile(q, 0, 4)
            msg_ref[2 * p + 1, 32 * q : 32 * q + 32, :] = tile(q, 5, 4)
        t0, t1, t2 = tile(0, 4), tile(1, 4), tile(2, 4)
        msg_ref[2 * p, 64:72, :] = jnp.where(sub < 4, t0, pltpu.roll(t1, 4, 0))
        msg_ref[2 * p + 1, 64:72, :] = jnp.where(sub < 4, pltpu.roll(t0, 4, 0), t1)
        msg_ref[2 * p, 72:80, :] = fours([tile(2, j) for j in range(4)])
        msg_ref[2 * p + 1, 72:80, :] = fours([tile(2, j) for j in range(5, 9)])
        msg_ref[2 * p, 80:84, :] = t2[0:4]
        msg_ref[2 * p + 1, 80:84, :] = pltpu.roll(t2, 4, 0)[0:4]
        return carry

    lax.fori_loop(0, NLATD // 2, pack, 0)


def face_below_row(first_row):
    row = lax.broadcasted_iota(jnp.int32, (8, 128), 0) * 0 + first_row
    below = jnp.sin(row.astype(F32) * np.float32(np.pi) / NLAT)
    return lanes9(below[0:1])


def polar_filter(mask_ref, cut_ref, full_ref, real_ref, s_ref, uh_ref, ul_ref, z_ref):
    rows = 3 * LEVD * ROWS
    flat = s_ref.reshape(rows, NLON)
    cos9 = [[np.float32(np.cos(2 * np.pi * a * k / 9)) for k in range(5)] for a in range(5)]
    sin9 = [[np.float32(np.sin(2 * np.pi * a * k / 9)) for k in range(5)] for a in range(5)]

    def forward(r, carry):
        at = pl.ds(pl.multiple_of(16 * r, 16), 16)
        v = [flat[at, 128 * a : 128 * a + 128] for a in range(RADIX)]
        even = [v[a] + v[9 - a] for a in range(1, 5)]
        odd = [v[a] - v[9 - a] for a in range(1, 5)]

        def put(slot, x):
            high, low = split_bf16(x)
            uh_ref[at, 128 * slot : 128 * slot + 128] = high
            ul_ref[at, 128 * slot : 128 * slot + 128] = low

        put(8, v[0] + ((even[0] + even[1]) + (even[2] + even[3])))
        for k in range(1, 5):
            put(2 * k - 2, v[0] + sum(even[a - 1] * cos9[a][k] for a in range(1, 5)))
            put(2 * k - 1, -sum(odd[a - 1] * sin9[a][k] for a in range(1, 5)))
        return carry

    lax.fori_loop(0, rows // 16, forward, 0)

    row24 = lax.broadcasted_iota(jnp.int32, (ROWS, 128), 0)
    lane24 = lax.broadcasted_iota(jnp.int32, (ROWS, 128), 1)
    cuts = jnp.full((ROWS, 128), 10000, jnp.int32)
    for r in range(ROWS):
        cuts = jnp.where(row24 == r, jnp.where(mask_ref[r] > 0, cut_ref[r], 10000), cuts)

    for k in range(1, 5):
        wave = k + RADIX * lane24
        keep = (jnp.minimum(wave, NLON - wave) >= cuts).astype(F32)
        keep = jnp.concatenate([jnp.concatenate([keep, keep], axis=1)] * 12, axis=0)
        at = pl.ds(256 * (k - 1), 256)
        tables_k = full_ref[0, k - 1], full_ref[1, k - 1]
        x = dot3(uh_ref[:, at], ul_ref[:, at], *tables_k, ((1,), (0,)))
        xh, xl = split_bf16(x * keep)
        z_ref[:, at] = dot3(xh, xl, *tables_k, ((1,), (1,)))
    wave = RADIX * jnp.where(lane24 <= 64, lane24, lane24 - 64)
    weight = jnp.where(jnp.logical_or(lane24 == 0, lane24 == 64), 1.0, 2.0)
    keep = jnp.concatenate([jnp.where(wave >= cuts, weight, 0.0)] * 12, axis=0)
    x = dot3(uh_ref[:, 1024:1152], ul_ref[:, 1024:1152], real_ref[0], real_ref[1], ((1,), (0,)))
    xh, xl = split_bf16(x * keep)
    z_ref[:, 1024:1152] = dot3(xh, xl, real_ref[0], real_ref[1], ((1,), (1,)))

    def backward(r, carry):
        at = pl.ds(pl.multiple_of(8 * r, 8), 8)
        z0 = z_ref[at, 1024:1152] * np.float32(1.0 / NLON)
        zr = [z_ref[at, 256 * k : 256 * k + 128] * np.float32(2.0 / NLON) for k in range(4)]
        zi = [z_ref[at, 256 * k + 128 : 256 * k + 256] * np.float32(2.0 / NLON) for k in range(4)]
        flat[at, 0:128] = flat[at, 0:128] - (z0 + ((zr[0] + zr[1]) + (zr[2] + zr[3])))
        for a in range(1, 5):
            even = z0 + sum(zr[k - 1] * cos9[a][k] for k in range(1, 5))
            odd = sum(zi[k - 1] * sin9[a][k] for k in range(1, 5))
            lo, hi = pl.ds(128 * a, 128), pl.ds(128 * (9 - a), 128)
            flat[at, lo] = flat[at, lo] - (even - odd)
            flat[at, hi] = flat[at, hi] - (even + odd)
        return carry

    lax.fori_loop(0, rows // 8, backward, 0)


STEPS = (0, 1, 7, 2, 6, 3, 5, 4)
ACROSS = (0, 1, 3, 2)


def exchange_kernel(msg_ref, sum_ref, out_ref, sums_ref, mid_ref, mid_sum, s1, r1, s2, r2, t1, q1, t2, q2, own):
    lat = lax.axis_index("lat")
    lev = lax.axis_index("lev")
    z, x = lat // NX, lax.rem(lat, NX)
    y = lev // 2

    barrier = pltpu.get_barrier_semaphore()

    def everyone(o, carry):
        pl.semaphore_signal(barrier, inc=1, device_id=(lax.rem(lat + o, NLATD), lev), device_id_type=MESH)
        return carry

    lax.fori_loop(1, NLATD, everyone, 0)

    def column(o, carry):
        pl.semaphore_signal(barrier, inc=1, device_id=(lat, lax.rem(lev + o, NLEVD)), device_id_type=MESH)
        return carry

    lax.fori_loop(1, NLEVD, column, 0)
    mine = pltpu.make_async_copy(msg_ref.at[lat], mid_ref.at[lat], own.at[0])
    mine.start()
    mine_sum = pltpu.make_async_copy(sum_ref, mid_sum.at[lat], own.at[1])
    mine_sum.start()
    pl.semaphore_wait(barrier, NLATD - 1 + NLEVD - 1)

    first = []
    for step in STEPS:
        dz = lax.rem(step + 2 * NZ - 2 * y, NZ)
        group = []
        for dx in ACROSS:
            to = lax.rem(z + dz, NZ) * NX + lax.rem(x + dx, NX)
            slot = 4 * step + dx
            big = pltpu.make_async_remote_copy(
                src_ref=msg_ref.at[to], dst_ref=mid_ref.at[lat], send_sem=s1.at[slot], recv_sem=r1.at[slot],
                device_id=(to, lev), device_id_type=MESH,
            )
            small = pltpu.make_async_remote_copy(
                src_ref=sum_ref, dst_ref=mid_sum.at[lat], send_sem=t1.at[slot], recv_sem=q1.at[slot],
                device_id=(to, lev), device_id_type=MESH,
            )
            group.append((big, small))
            if dx == 0:
                remote = dz != 0

                @pl.when(remote)
                def _():
                    big.start()
                    small.start()
            else:
                big.start()
                small.start()
        first.append((dz, group))

    second = []
    for dz, group in first:
        source = lax.rem(z + NZ - dz, NZ)
        for n, (big, small) in enumerate(group):
            if n == 0:
                @pl.when(dz != 0)
                def _():
                    big.wait_recv()

                @pl.when(dz == 0)
                def _():
                    mine.wait()
            else:
                big.wait_recv()
        piece = mid_ref.at[pl.ds(NX * source, NX)]
        away = pltpu.make_async_remote_copy(
            src_ref=piece, dst_ref=out_ref.at[lev], send_sem=s2.at[source], recv_sem=r2.at[lev],
            device_id=(lat, source), device_id_type=MESH,
        )
        local = pltpu.make_async_copy(piece, out_ref.at[lev], own.at[2])

        @pl.when(source != lev)
        def _():
            away.start()

        @pl.when(source == lev)
        def _():
            local.start()

        second.append((source, away, local))

    for dz, group in first:
        for n, (big, small) in enumerate(group):
            if n == 0:
                @pl.when(dz != 0)
                def _():
                    small.wait_recv()
                    big.wait_send()
                    small.wait_send()
            else:
                small.wait_recv()
                big.wait_send()
                small.wait_send()
    mine_sum.wait()
    spread = []
    for o in range(1, NLEVD):
        to = lax.rem(lev + o, NLEVD)
        copy = pltpu.make_async_remote_copy(
            src_ref=mid_sum, dst_ref=sums_ref.at[lev], send_sem=t2.at[o], recv_sem=q2.at[o],
            device_id=(lat, to), device_id_type=MESH,
        )
        copy.start()
        spread.append(copy)
    keep_sum = pltpu.make_async_copy(mid_sum, sums_ref.at[lev], own.at[3])
    keep_sum.start()

    for source, away, local in second:
        @pl.when(source != lev)
        def _():
            away.wait_send()

        @pl.when(source == lev)
        def _():
            local.wait()
    for o in range(1, NLEVD):
        sender = lax.rem(lev + o, NLEVD)
        pltpu.make_async_remote_copy(
            src_ref=mid_ref.at[pl.ds(0, NX)], dst_ref=out_ref.at[sender], send_sem=s2.at[sender],
            recv_sem=r2.at[sender], device_id=(lat, sender), device_id_type=MESH,
        ).wait_recv()
    for copy in spread:
        copy.wait()
    keep_sum.wait()


def remap_kernel(in_ref, sums_ref, weight_ref, target_ref, thick_ref, temp_ref, tracer_ref, r_ref):
    lat = lax.axis_index("lat")
    lane = lax.broadcasted_iota(jnp.int32, (8, 128), 1)

    def merge(parts):
        return jnp.where(
            lane < 48, jnp.where(lane < 24, parts[0], parts[1]), jnp.where(lane < 72, parts[2], parts[3])
        )

    def move(v, source, target):
        amount = (target - source) % 128
        return v if amount == 0 else pltpu.roll(v, amount, 1)

    phase = jnp.where(lane >= 72, lane - 72, jnp.where(lane >= 48, lane - 48, jnp.where(lane >= 24, lane - 24, lane)))

    def unpack(g, carry):
        for j in range(5):
            if j < 4:
                one = [in_ref[g, x, 8 * j : 8 * j + 8, :] for x in range(4)]
                two = [in_ref[g, x, 32 + 8 * j : 40 + 8 * j, :] for x in range(4)]
                last = [in_ref[g, x, 72:80, :] for x in range(4)]
                lane0 = 32 * j
            else:
                one = [in_ref[g, x, 64:72, :] for x in range(4)]
                two = [pltpu.roll(v, 4, 0) for v in one]
                last = [in_ref[g, x, 80:84, :] for x in range(4)]
                last = [jnp.concatenate([v, v], axis=0) for v in last]
                lane0 = 0

            def put(fl, v):
                f, l = fl // 4, fl % 4
                r_ref[f, g * 4 + l, 8 * j : 8 * j + 8, :] = v

            for n in range(5):
                put(n, merge([move(one[x], 24 * n, 24 * x) for x in range(4)]))
                put(5 + n, merge([move(two[x], 24 * n, 24 * x) for x in range(4)]))
            put(10, merge([move(last[x], lane0, 24 * x) for x in range(4)]))
            a = merge([move(one[x], 120, 24 * x) for x in range(4)])
            b = merge([move(two[x], 120, 24 * x + 8) for x in range(4)])
            c = merge([move(last[x], lane0 + 24, 24 * x + 16) for x in range(4)])
            put(11, jnp.where(phase < 8, a, jnp.where(phase < 16, b, c)))
        return carry

    lax.fori_loop(0, NLEVD, unpack, 0)

    area = float(np.sum(np.sin((np.arange(NLAT) + 0.5) * np.pi / NLAT)))
    total = jnp.sum(jnp.sum(sums_ref[...], axis=0, keepdims=True), axis=1, keepdims=True)
    scale = target_ref[0] * (NLON * area) / total
    scale = jnp.broadcast_to(scale, (8, 128))
    weights = [weight_ref[k] for k in range(LEV)]
    whole = weights[0]
    for k in range(1, LEV):
        whole = whole + weights[k]
    odd = lax.rem(lat, 2)

    def tile(j, count, lon0):
        at = pl.ds(pl.multiple_of(8 * j, 8), 8)
        surface = r_ref[0, 0, at, :]
        for m in range(1, LEV):
            surface = surface + r_ref[0, m, at, :]
        unit = surface / jnp.full((8, 128), whole)
        previous = (jnp.zeros((8, 128), F32), jnp.zeros((8, 128), F32))
        running = None
        for k0 in range(0, LEV, 8):
            bounds = []
            for k in range(k0, k0 + 8):
                running = weights[k] if running is None else running + weights[k]
                bounds.append(unit * running)
            temps = [jnp.zeros((8, 128), F32)] * 8
            tracs = [jnp.zeros((8, 128), F32)] * 8
            top = jnp.zeros((8, 128), F32)
            for m in range(LEV):
                th = r_ref[0, m, at, :]
                te = r_ref[1, m, at, :]
                tr = r_ref[2, m, at, :]
                for n in range(8):
                    part = jnp.minimum(jnp.maximum(bounds[n] - top, 0.0), th)
                    temps[n] = temps[n] + te * part
                    tracs[n] = tracs[n] + tr * part
                top = top + th
            for n in range(8):
                k = k0 + n
                target = unit * weights[k]
                inverse = 1.0 / target
                rows = pl.ds(lon0 * LEV + k, count, stride=LEV)
                thick_ref[rows, :] = (target * scale)[0:count, 0:96]
                temp_ref[rows, :] = ((temps[n] - previous[0]) * inverse)[0:count, 0:96]
                tracer_ref[rows, :] = ((tracs[n] - previous[1]) * inverse)[0:count, 0:96]
                previous = (temps[n], tracs[n])

    def full(j, carry):
        tile(j, 8, 8 * j + 4 * odd)
        return carry

    lax.fori_loop(0, 4, full, 0)
    tile(4, 4, 32 - 32 * odd)


def on_device(th, te, tr, ec, nc, polar_mask, wave_cutoff, level_weight, target_surface):
    vmem = pl.BlockSpec(memory_space=pltpu.VMEM)
    smem = pl.BlockSpec(memory_space=pltpu.SMEM)
    hbm = pl.BlockSpec(memory_space=pl.ANY)
    full, real = tables()
    msg, part = pl.pallas_call(
        dynamics_kernel,
        name="dynamics",
        out_shape=(
            jax.ShapeDtypeStruct((NLATD, SENT, 128), F32),
            jax.ShapeDtypeStruct((1, 128), F32),
        ),
        in_specs=[vmem] * 5 + [smem] * 2 + [vmem] * 2,
        out_specs=(vmem, vmem),
        scratch_shapes=[
            pltpu.VMEM((3, LEVD, ROWS, NLON), F32),
            pltpu.VMEM((16, NLON), F32),
            pltpu.VMEM((12, NLON), F32),
            pltpu.VMEM((16, NLON), F32),
            pltpu.VMEM((12, NLON), F32),
            pltpu.VMEM((288, NLON), BF16),
            pltpu.VMEM((288, NLON), BF16),
            pltpu.VMEM((288, NLON), F32),
            pltpu.VMEM((3, NLON, 128), F32),
            pltpu.SemaphoreType.DMA((2,)),
            pltpu.SemaphoreType.DMA((2,)),
        ],
        compiler_params=pltpu.CompilerParams(collective_id=0, has_side_effects=True),
    )(th, te, tr, ec, nc, polar_mask, wave_cutoff, jnp.asarray(full), jnp.asarray(real))
    columns, sums = pl.pallas_call(
        exchange_kernel,
        name="exchange",
        out_shape=(
            jax.ShapeDtypeStruct((NLEVD, NX, SENT, 128), F32),
            jax.ShapeDtypeStruct((NLEVD, NLATD, 1, 128), F32),
        ),
        in_specs=[hbm, vmem],
        out_specs=(hbm, hbm),
        scratch_shapes=[
            pltpu.VMEM((NLATD, SENT, 128), F32),
            pltpu.VMEM((NLATD, 1, 128), F32),
            pltpu.SemaphoreType.DMA((32,)),
            pltpu.SemaphoreType.DMA((32,)),
            pltpu.SemaphoreType.DMA((8,)),
            pltpu.SemaphoreType.DMA((8,)),
            pltpu.SemaphoreType.DMA((32,)),
            pltpu.SemaphoreType.DMA((32,)),
            pltpu.SemaphoreType.DMA((8,)),
            pltpu.SemaphoreType.DMA((8,)),
            pltpu.SemaphoreType.DMA((4,)),
        ],
        compiler_params=pltpu.CompilerParams(collective_id=1, has_side_effects=True),
    )(msg, part)
    outs = pl.pallas_call(
        remap_kernel,
        name="remap",
        out_shape=tuple(jax.ShapeDtypeStruct((36 * LEV, 96), F32) for _ in range(3)),
        in_specs=[vmem, vmem, smem, smem],
        out_specs=(vmem, vmem, vmem),
        scratch_shapes=[pltpu.VMEM((3, LEV, 40, 128), F32)],
    )(columns, sums.reshape(NLEVD * NLATD, 128), level_weight, target_surface)
    return tuple(o.reshape(36, LEV, 96).transpose(1, 2, 0) for o in outs)


def solution(mesh):
    field = P("lev", "lat", None)
    return jax.shard_map(
        on_device,
        mesh=mesh,
        in_specs=(field,) * 5 + (P("lat"), P("lat"), P(), P()),
        out_specs=(P(None, "lev", "lat"),) * 3,
        check_vma=False,
    )
```

```python
import functools

import jax
import jax.numpy as jnp
import numpy as np
from jax import lax
from jax.experimental import pallas as pl
from jax.experimental.pallas import tpu as pltpu
from jax.sharding import PartitionSpec as P

MESH = pl.DeviceIdType.MESH
F32 = jnp.float32
BF16 = jnp.bfloat16

NLON, NLAT, LEV = 1152, 768, 32
ROWS = 24
LEVD = 4
NZ, NX, NY = 8, 4, 4
NLATD, NLEVD = 32, 8
RADIX, POINTS = 9, 128
SENT = 84
POLAR_BANDS = -(-(NLAT // 5) // ROWS)


def split_bf16(x):
    high = x.astype(BF16)
    return high, (x - high.astype(F32)).astype(BF16)


def tables():
    b = np.arange(POINTS)[:, None]
    full = np.zeros((4, 256, 256))
    for k1 in range(1, 5):
        angle = 2.0 * np.pi * ((b * (k1 + RADIX * np.arange(POINTS)[None, :])) % NLON) / NLON
        c, s = np.cos(angle), np.sin(angle)
        full[k1 - 1] = np.block([[c, -s], [s, c]])
    col = np.arange(POINTS)[None, :]
    wave = np.where(col <= 64, col, col - 64)
    angle = 2.0 * np.pi * ((b * wave) % POINTS) / POINTS
    real = np.where(col <= 64, np.cos(angle), np.sin(angle))

    def pair(x):
        high = x.astype(np.float32).astype(BF16)
        low = (x - high.astype(np.float64)).astype(np.float32).astype(BF16)
        return np.stack([np.asarray(high), np.asarray(low)])

    return pair(full), pair(real)


def dot3(xh, xl, th, tl, dims):
    dot = functools.partial(
        lax.dot_general, dimension_numbers=(dims, ((), ())), preferred_element_type=F32
    )
    return dot(xh, th) + dot(xl, th) + dot(xh, tl)


def lanes9(x):
    return jnp.concatenate([x] * RADIX, axis=1)


def step_kernel(
    th_hbm, te_hbm, tr_hbm, ec_hbm, nc_hbm, mask_ref, cut_ref, weight_ref, target_ref, full_hbm, real_hbm,
    thick_ref, temp_ref, tracer_ref,
    in_ref, full_ref, real_ref, s_ref, up_ref, down_ref, from_south, from_north, uh_ref, ul_ref, z_ref, t_ref,
    msg_ref, mid_ref, col_ref, part_ref, ring_sum, all_sum, r_ref,
    load_sem, halo_send, halo_recv, own_sem, zs, zr, ps, pr, rs, rr, fs, fr,
):
    lat = lax.axis_index("lat")
    lev = lax.axis_index("lev")
    z, x = lat // NX, lax.rem(lat, NX)
    north = lax.rem(lat + 1, NLATD)
    south = lax.rem(lat + NLATD - 1, NLATD)
    polar = jnp.logical_or(lat < POLAR_BANDS, lat >= NLATD - POLAR_BANDS)

    barrier = pltpu.get_barrier_semaphore()
    for other in (north, south):
        pl.semaphore_signal(barrier, inc=1, device_id=(other, lev), device_id_type=MESH)

    def plane_peer(o):
        return z * NX + lax.rem(x + o // NLEVD, NX), lax.rem(lev + o, NLEVD)

    def greet_plane(o, carry):
        pl.semaphore_signal(barrier, inc=1, device_id=plane_peer(o), device_id_type=MESH)
        return carry

    def greet_ring(o, carry):
        peer = (lax.rem(lat + NX * o, NLATD), lev)
        pl.semaphore_signal(barrier, inc=1, device_id=peer, device_id_type=MESH)
        return carry

    lax.fori_loop(1, NZ, greet_ring, 0)
    lax.fori_loop(1, NX * NLEVD, greet_plane, 0)

    fields_hbm = (th_hbm, te_hbm, tr_hbm, nc_hbm, ec_hbm)
    loads = [pltpu.make_async_copy(fields_hbm[f], in_ref.at[f], load_sem.at[f]) for f in range(5)]
    for load in loads:
        load.start()
    table_loads = (
        pltpu.make_async_copy(full_hbm, full_ref, load_sem.at[5]),
        pltpu.make_async_copy(real_hbm, real_ref, load_sem.at[6]),
    )

    @pl.when(polar)
    def _():
        for load in table_loads:
            load.start()

    for load in loads:
        load.wait()
    th_ref, te_ref, tr_ref, nc_ref, ec_ref = (in_ref.at[f] for f in range(5))
    fields = (th_ref, te_ref, tr_ref, nc_ref)
    for f in range(4):
        for l in range(LEVD):
            up_ref[pl.ds(4 * f + l, 1), :] = fields[f][l, ROWS - 1 : ROWS, :]
            if f < 3:
                down_ref[pl.ds(4 * f + l, 1), :] = fields[f][l, 0:1, :]

    def east(l, carry):
        th, te, tr = th_ref[l], te_ref[l], tr_ref[l]
        mass = ec_ref[l] * (th + pltpu.roll(th, NLON - 1, 1)) * 0.5
        temp = mass * (te + pltpu.roll(te, NLON - 1, 1)) * 0.5
        trac = mass * (tr + pltpu.roll(tr, NLON - 1, 1)) * 0.5
        s_ref[0, l] = pltpu.roll(mass, 1, 1) - mass
        s_ref[1, l] = pltpu.roll(temp, 1, 1) - temp
        s_ref[2, l] = pltpu.roll(trac, 1, 1) - trac
        return carry

    lax.fori_loop(0, LEVD, east, 0)

    pl.semaphore_wait(barrier, 2 + NZ - 1 + NX * NLEVD - 1)
    to_north = pltpu.make_async_remote_copy(
        src_ref=up_ref, dst_ref=from_south, send_sem=halo_send.at[0], recv_sem=halo_recv.at[0],
        device_id=(north, lev), device_id_type=MESH,
    )
    to_south = pltpu.make_async_remote_copy(
        src_ref=down_ref, dst_ref=from_north, send_sem=halo_send.at[1], recv_sem=halo_recv.at[1],
        device_id=(south, lev), device_id_type=MESH,
    )
    to_north.start()
    to_south.start()

    first_row = lat * ROWS
    row = (first_row + lax.broadcasted_iota(jnp.int32, (ROWS, 128), 0)).astype(F32)
    center = lanes9(jnp.sin((row + 0.5) * np.float32(np.pi) / NLAT))
    face = lanes9(jnp.sin((row + 1.0) * np.float32(np.pi) / NLAT))
    face_below = face_below_row(first_row)
    inverse_center = 1.0 / center
    row_in = lax.broadcasted_iota(jnp.int32, (ROWS, NLON), 0)

    to_north.wait()
    to_south.wait()

    for l in range(LEVD):
        th, te, tr = th_ref[l], te_ref[l], tr_ref[l]

        def above(v, f):
            edge = from_north[4 * f + l : 4 * f + l + 1, :]
            edge = jnp.where(lat == NLATD - 1, 0.0, edge)
            return jnp.where(row_in == ROWS - 1, edge, pltpu.roll(v, ROWS - 1, 0))

        def south_row(f):
            return from_south[4 * f + l : 4 * f + l + 1, :]

        mass = nc_ref[l] * (th + above(th, 0)) * 0.5 * face
        temp = mass * (te + above(te, 1)) * 0.5
        trac = mass * (tr + above(tr, 2)) * 0.5
        mass_s = south_row(3) * (south_row(0) + th[0:1]) * 0.5 * face_below
        temp_s = mass_s * (south_row(1) + te[0:1]) * 0.5
        trac_s = mass_s * (south_row(2) + tr[0:1]) * 0.5
        for f, (flux, below) in enumerate(((mass, mass_s), (temp, temp_s), (trac, trac_s))):
            lower = jnp.where(row_in == 0, below, pltpu.roll(flux, 1, 0))
            s_ref[f, l] = s_ref[f, l] - (flux - lower) * inverse_center

    @pl.when(polar)
    def _():
        for load in table_loads:
            load.wait()
        polar_filter(mask_ref, cut_ref, full_ref, real_ref, s_ref, uh_ref, ul_ref, z_ref)

    def update(l, total):
        th, te, tr = th_ref[l], te_ref[l], tr_ref[l]
        mass = s_ref[0, l]
        inverse = 1.0 / th
        new_th = th + mass
        s_ref[0, l] = new_th
        s_ref[1, l] = te + (s_ref[1, l] - te * mass) * inverse
        s_ref[2, l] = tr + (s_ref[2, l] - tr * mass) * inverse
        weighted = new_th * center
        for a in range(RADIX):
            part = weighted[:, 128 * a : 128 * a + 128]
            total = total + (part[0:8] + part[8:16] + part[16:24])
        return total

    total = lax.fori_loop(0, LEVD, update, jnp.zeros((8, 128), F32))
    total = jnp.sum(total, axis=0, keepdims=True)
    part_ref[...] = total
    ring_sum[z] = total

    flat = s_ref.reshape(3 * LEVD * ROWS, NLON)
    for a in range(RADIX):
        at = pl.ds(128 * a, 128)
        one = jnp.concatenate([flat[0:120, at], flat[264:272, at]], axis=0)
        two = jnp.concatenate([flat[120:240, at], flat[272:280, at]], axis=0)
        last = jnp.concatenate([flat[240:264, at], flat[280:288, at]], axis=0)
        t_ref[0, at, :] = one.T
        t_ref[1, at, :] = two.T
        t_ref[2, at, :] = jnp.concatenate([last] * 4, axis=0).T

    sub = lax.broadcasted_iota(jnp.int32, (8, 128), 0)
    lane = lax.broadcasted_iota(jnp.int32, (8, 128), 1)

    def pack(p, carry):
        base = 72 * p

        def tile(q, j, n=1):
            return t_ref[q, pl.ds(pl.multiple_of(base + 8 * j, 8), 8 * n), :]

        def fours(u):
            return jnp.where(
                lane < 64, jnp.where(lane < 32, u[0], u[1]), jnp.where(lane < 96, u[2], u[3])
            )

        for q in range(2):
            for half in range(2):
                at = pl.ds(40 * half + 16 * q, 16)
                msg_ref[2 * p, at, :] = tile(q, 2 * half, 2)
                msg_ref[2 * p + 1, at, :] = tile(q, 5 + 2 * half, 2)
        t0, t1, t2 = tile(0, 4), tile(1, 4), tile(2, 4)
        msg_ref[2 * p, 72:80, :] = jnp.where(sub < 4, t0, pltpu.roll(t1, 4, 0))
        msg_ref[2 * p + 1, 72:80, :] = jnp.where(sub < 4, pltpu.roll(t0, 4, 0), t1)
        msg_ref[2 * p, 32:40, :] = fours([tile(2, j) for j in range(4)])
        msg_ref[2 * p + 1, 32:40, :] = fours([tile(2, j) for j in range(5, 9)])
        msg_ref[2 * p, 80:84, :] = t2[0:4]
        msg_ref[2 * p + 1, 80:84, :] = pltpu.roll(t2, 4, 0)[0:4]
        return carry

    lax.fori_loop(0, NLATD // 2, pack, 0)

    def ring_part(o):
        return pltpu.make_async_remote_copy(
            src_ref=part_ref, dst_ref=ring_sum.at[z], send_sem=ps.at[o], recv_sem=pr.at[o],
            device_id=(lax.rem(lat + NX * o, NLATD), lev), device_id_type=MESH,
        )

    def plane_part(o):
        return pltpu.make_async_remote_copy(
            src_ref=ring_sum, dst_ref=all_sum.at[x * NLEVD + lev], send_sem=rs.at[o], recv_sem=rr.at[o],
            device_id=plane_peer(o), device_id_type=MESH,
        )

    def each(count, action, start=0):
        def body(o, carry):
            action(o)
            return carry

        lax.fori_loop(start, count, body, 0)

    each(NZ, lambda o: ring_part(o).start(), 1)

    def distance(k):
        return jnp.where(lax.rem(k, 2) == 1, (k + 1) // 2, lax.rem(NZ - k // 2, NZ))

    def along_z(chunk, k):
        to = lax.rem(z + distance(k), NZ)
        first, count = CHUNKS[chunk]
        return pltpu.make_async_remote_copy(
            src_ref=msg_ref.at[pl.ds(NX * to, NX), pl.ds(first, count)],
            dst_ref=mid_ref.at[pl.ds(NX * z, NX), pl.ds(first, count)],
            send_sem=zs.at[chunk, k], recv_sem=zr.at[chunk, k],
            device_id=(to * NX + x, lev), device_id_type=MESH,
        )

    for chunk in range(len(CHUNKS)):
        each(NZ, lambda k: along_z(chunk, k).start(), 1)
    mine = pltpu.make_async_copy(
        msg_ref.at[pl.ds(NX * z, NX)], mid_ref.at[pl.ds(NX * z, NX)], own_sem.at[0]
    )
    mine.start()

    each(NZ, lambda o: ring_part(o).wait_recv(), 1)
    each(NX * NLEVD, lambda o: plane_part(o).start(), 1)
    mine.wait()

    def onward(chunk, source, to_x):
        first, count = CHUNKS[chunk]
        piece = mid_ref.at[NX * source + to_x, pl.ds(first, count)]
        place = col_ref.at[lev, x, pl.ds(first, count)]
        away = pltpu.make_async_remote_copy(
            src_ref=piece, dst_ref=place, send_sem=fs.at[chunk, NX * source + to_x],
            recv_sem=fr.at[chunk, NX * lev + x],
            device_id=(z * NX + to_x, source), device_id_type=MESH,
        )
        stay = pltpu.make_async_copy(piece, place, own_sem.at[1 + chunk])
        return away, stay

    def forward(chunk, k):
        source = lax.rem(z + NZ - distance(k), NZ)

        @pl.when(k > 0)
        def _():
            along_z(chunk, k).wait_recv()

        for dx in ACROSS:
            away, stay = onward(chunk, source, lax.rem(x + dx, NX))
            if dx == 0:
                pl.when(source != lev)(away.start)
                pl.when(source == lev)(stay.start)
            else:
                away.start()

    def arrived(chunk):
        first, count = CHUNKS[chunk]

        def one(n):
            here = jnp.logical_and(n // NX == lev, lax.rem(n, NX) == x)
            away = pltpu.make_async_remote_copy(
                src_ref=mid_ref.at[0, pl.ds(first, count)],
                dst_ref=col_ref.at[n // NX, lax.rem(n, NX), pl.ds(first, count)],
                send_sem=fs.at[chunk, n], recv_sem=fr.at[chunk, n],
                device_id=(z * NX + lax.rem(n, NX), n // NX), device_id_type=MESH,
            )
            pl.when(jnp.logical_not(here))(away.wait_recv)

        each(NX * NLEVD, one)
        away, stay = onward(chunk, lev, x)
        stay.wait()

    remap = Remap(lat, lane, col_ref, r_ref, weight_ref, target_ref, thick_ref, temp_ref, tracer_ref)

    each(NZ, lambda k: forward(0, k))
    each(4, lambda k: forward(1, k))
    each(NX * NLEVD, lambda o: plane_part(o).wait_recv(), 1)
    all_sum[x * NLEVD + lev] = ring_sum[...]
    remap.set_scale(all_sum)
    arrived(0)
    remap.unpack((0, 1))

    def tiles_a(j):
        remap.tile(j)
        forward(1, 4 + 2 * j)
        forward(1, 5 + 2 * j)

    each(2, tiles_a)
    each(4, lambda k: forward(2, k))
    arrived(1)
    remap.unpack((2, 3))

    def tiles_b(j):
        remap.tile(2 + j)
        forward(2, 4 + 2 * j)
        forward(2, 5 + 2 * j)

    each(2, tiles_b)
    arrived(2)
    remap.unpack((4,))
    remap.half_tile()

    each(NZ, lambda o: ring_part(o).wait_send(), 1)
    each(NX * NLEVD, lambda o: plane_part(o).wait_send(), 1)
    for chunk in range(len(CHUNKS)):
        each(NZ, lambda k: along_z(chunk, k).wait_send(), 1)

        def sent(n):
            here = jnp.logical_and(n // NX == lev, lax.rem(n, NX) == x)
            away, stay = onward(chunk, n // NX, lax.rem(n, NX))
            pl.when(jnp.logical_not(here))(away.wait_send)

        each(NX * NLEVD, sent)


def face_below_row(first_row):
    row = lax.broadcasted_iota(jnp.int32, (8, 128), 0) * 0 + first_row
    below = jnp.sin(row.astype(F32) * np.float32(np.pi) / NLAT)
    return lanes9(below[0:1])


def polar_filter(mask_ref, cut_ref, full_ref, real_ref, s_ref, uh_ref, ul_ref, z_ref):
    rows = 3 * LEVD * ROWS
    flat = s_ref.reshape(rows, NLON)
    cos9 = [[np.float32(np.cos(2 * np.pi * a * k / 9)) for k in range(5)] for a in range(5)]
    sin9 = [[np.float32(np.sin(2 * np.pi * a * k / 9)) for k in range(5)] for a in range(5)]

    def forward(r, carry):
        at = pl.ds(pl.multiple_of(16 * r, 16), 16)
        v = [flat[at, 128 * a : 128 * a + 128] for a in range(RADIX)]
        even = [v[a] + v[9 - a] for a in range(1, 5)]
        odd = [v[a] - v[9 - a] for a in range(1, 5)]

        def put(slot, x):
            high, low = split_bf16(x)
            uh_ref[at, 128 * slot : 128 * slot + 128] = high
            ul_ref[at, 128 * slot : 128 * slot + 128] = low

        put(8, v[0] + ((even[0] + even[1]) + (even[2] + even[3])))
        for k in range(1, 5):
            put(2 * k - 2, v[0] + sum(even[a - 1] * cos9[a][k] for a in range(1, 5)))
            put(2 * k - 1, -sum(odd[a - 1] * sin9[a][k] for a in range(1, 5)))
        return carry

    lax.fori_loop(0, rows // 16, forward, 0)

    row24 = lax.broadcasted_iota(jnp.int32, (ROWS, 128), 0)
    lane24 = lax.broadcasted_iota(jnp.int32, (ROWS, 128), 1)
    cuts = jnp.full((ROWS, 128), 10000, jnp.int32)
    for r in range(ROWS):
        cuts = jnp.where(row24 == r, jnp.where(mask_ref[r] > 0, cut_ref[r], 10000), cuts)

    for k in range(1, 5):
        wave = k + RADIX * lane24
        keep = (jnp.minimum(wave, NLON - wave) >= cuts).astype(F32)
        keep = jnp.concatenate([jnp.concatenate([keep, keep], axis=1)] * 12, axis=0)
        at = pl.ds(256 * (k - 1), 256)
        tables_k = full_ref[0, k - 1], full_ref[1, k - 1]
        x = dot3(uh_ref[:, at], ul_ref[:, at], *tables_k, ((1,), (0,)))
        xh, xl = split_bf16(x * keep)
        z_ref[:, at] = dot3(xh, xl, *tables_k, ((1,), (1,)))
    wave = RADIX * jnp.where(lane24 <= 64, lane24, lane24 - 64)
    weight = jnp.where(jnp.logical_or(lane24 == 0, lane24 == 64), 1.0, 2.0)
    keep = jnp.concatenate([jnp.where(wave >= cuts, weight, 0.0)] * 12, axis=0)
    x = dot3(uh_ref[:, 1024:1152], ul_ref[:, 1024:1152], real_ref[0], real_ref[1], ((1,), (0,)))
    xh, xl = split_bf16(x * keep)
    z_ref[:, 1024:1152] = dot3(xh, xl, real_ref[0], real_ref[1], ((1,), (1,)))

    def backward(r, carry):
        at = pl.ds(pl.multiple_of(8 * r, 8), 8)
        z0 = z_ref[at, 1024:1152] * np.float32(1.0 / NLON)
        zr = [z_ref[at, 256 * k : 256 * k + 128] * np.float32(2.0 / NLON) for k in range(4)]
        zi = [z_ref[at, 256 * k + 128 : 256 * k + 256] * np.float32(2.0 / NLON) for k in range(4)]
        flat[at, 0:128] = flat[at, 0:128] - (z0 + ((zr[0] + zr[1]) + (zr[2] + zr[3])))
        for a in range(1, 5):
            even = z0 + sum(zr[k - 1] * cos9[a][k] for k in range(1, 5))
            odd = sum(zi[k - 1] * sin9[a][k] for k in range(1, 5))
            lo, hi = pl.ds(128 * a, 128), pl.ds(128 * (9 - a), 128)
            flat[at, lo] = flat[at, lo] - (even - odd)
            flat[at, hi] = flat[at, hi] - (even + odd)
        return carry

    lax.fori_loop(0, rows // 8, backward, 0)


ACROSS = (0, 1, 3, 2)
CHUNKS = ((0, 40), (40, 32), (72, 12))


class Remap:
    def __init__(self, lat, lane, col_ref, r_ref, weight_ref, target_ref, thick_ref, temp_ref, tracer_ref):
        self.odd = lax.rem(lat, 2)
        self.lane = lane
        self.col_ref, self.r_ref, self.target_ref = col_ref, r_ref, target_ref
        self.outs = thick_ref, temp_ref, tracer_ref
        self.weights = [weight_ref[k] for k in range(LEV)]
        whole = self.weights[0]
        for k in range(1, LEV):
            whole = whole + self.weights[k]
        self.whole = whole

    def set_scale(self, all_sum):
        area = float(np.sum(np.sin((np.arange(NLAT) + 0.5) * np.pi / NLAT)))
        total = jnp.sum(all_sum[...].reshape(NX * NLEVD * NZ, 128), axis=0, keepdims=True)
        total = jnp.sum(total, axis=1, keepdims=True)
        self.scale = jnp.broadcast_to(self.target_ref[0] * (NLON * area) / total, (8, 128))

    def unpack(self, tiles):
        lane, col_ref, r_ref = self.lane, self.col_ref, self.r_ref

        def merge(parts):
            return jnp.where(
                lane < 48, jnp.where(lane < 24, parts[0], parts[1]), jnp.where(lane < 72, parts[2], parts[3])
            )

        def move(v, source, target):
            amount = (target - source) % 128
            return v if amount == 0 else pltpu.roll(v, amount, 1)

        phase = jnp.where(
            lane >= 72, lane - 72, jnp.where(lane >= 48, lane - 48, jnp.where(lane >= 24, lane - 24, lane))
        )

        def body(g, carry):
            for j in tiles:
                if j < 4:
                    row = 40 * (j // 2) + 8 * (j % 2)
                    one = [col_ref[g, x, row : row + 8, :] for x in range(4)]
                    two = [col_ref[g, x, row + 16 : row + 24, :] for x in range(4)]
                    last = [col_ref[g, x, 32:40, :] for x in range(4)]
                    lane0 = 32 * j
                else:
                    one = [col_ref[g, x, 72:80, :] for x in range(4)]
                    two = [pltpu.roll(v, 4, 0) for v in one]
                    last = [col_ref[g, x, 80:84, :] for x in range(4)]
                    last = [jnp.concatenate([v, v], axis=0) for v in last]
                    lane0 = 0

                def put(fl, v):
                    r_ref[fl // 4, g * 4 + fl % 4, 8 * j : 8 * j + 8, :] = v

                for n in range(5):
                    put(n, merge([move(one[x], 24 * n, 24 * x) for x in range(4)]))
                    put(5 + n, merge([move(two[x], 24 * n, 24 * x) for x in range(4)]))
                put(10, merge([move(last[x], lane0, 24 * x) for x in range(4)]))
                a = merge([move(one[x], 120, 24 * x) for x in range(4)])
                b = merge([move(two[x], 120, 24 * x + 8) for x in range(4)])
                c = merge([move(last[x], lane0 + 24, 24 * x + 16) for x in range(4)])
                put(11, jnp.where(phase < 8, a, jnp.where(phase < 16, b, c)))
            return carry

        lax.fori_loop(0, NLEVD, body, 0)

    def tile(self, j):
        self.columns(j, 8, 8 * j + 4 * self.odd)

    def half_tile(self):
        self.columns(4, 4, 32 - 32 * self.odd)

    def columns(self, j, count, lon0):
        weights, r_ref = self.weights, self.r_ref
        thick_ref, temp_ref, tracer_ref = self.outs
        at = pl.ds(pl.multiple_of(8 * j, 8), 8)
        surface = r_ref[0, 0, at, :]
        for m in range(1, LEV):
            surface = surface + r_ref[0, m, at, :]
        unit = surface / jnp.full((8, 128), self.whole)
        previous = (jnp.zeros((8, 128), F32), jnp.zeros((8, 128), F32))
        running = None
        for k0 in range(0, LEV, 8):
            bounds = []
            for k in range(k0, k0 + 8):
                running = weights[k] if running is None else running + weights[k]
                bounds.append(unit * running)
            temps = [jnp.zeros((8, 128), F32)] * 8
            tracs = [jnp.zeros((8, 128), F32)] * 8
            top = jnp.zeros((8, 128), F32)
            for m in range(LEV):
                th = r_ref[0, m, at, :]
                te = r_ref[1, m, at, :]
                tr = r_ref[2, m, at, :]
                for n in range(8):
                    part = jnp.minimum(jnp.maximum(bounds[n] - top, 0.0), th)
                    temps[n] = temps[n] + te * part
                    tracs[n] = tracs[n] + tr * part
                top = top + th
            for n in range(8):
                k = k0 + n
                target = unit * weights[k]
                inverse = 1.0 / target
                rows = pl.ds(lon0 * LEV + k, count, stride=LEV)
                thick_ref[rows, :] = (target * self.scale)[0:count, 0:96]
                temp_ref[rows, :] = ((temps[n] - previous[0]) * inverse)[0:count, 0:96]
                tracer_ref[rows, :] = ((tracs[n] - previous[1]) * inverse)[0:count, 0:96]
                previous = (temps[n], tracs[n])


def on_device(th, te, tr, ec, nc, polar_mask, wave_cutoff, level_weight, target_surface):
    vmem = pl.BlockSpec(memory_space=pltpu.VMEM)
    smem = pl.BlockSpec(memory_space=pltpu.SMEM)
    hbm = pl.BlockSpec(memory_space=pl.ANY)
    full, real = tables()
    dma = pltpu.SemaphoreType.DMA
    chunks = len(CHUNKS)
    outs = pl.pallas_call(
        step_kernel,
        name="step",
        out_shape=tuple(jax.ShapeDtypeStruct((36 * LEV, 96), F32) for _ in range(3)),
        in_specs=[hbm] * 5 + [smem] * 4 + [hbm] * 2,
        out_specs=(vmem, vmem, vmem),
        scratch_shapes=[
            pltpu.VMEM((5, LEVD, ROWS, NLON), F32),
            pltpu.VMEM(full.shape, BF16),
            pltpu.VMEM(real.shape, BF16),
            pltpu.VMEM((3, LEVD, ROWS, NLON), F32),
            pltpu.VMEM((16, NLON), F32),
            pltpu.VMEM((12, NLON), F32),
            pltpu.VMEM((16, NLON), F32),
            pltpu.VMEM((12, NLON), F32),
            pltpu.VMEM((288, NLON), BF16),
            pltpu.VMEM((288, NLON), BF16),
            pltpu.VMEM((288, NLON), F32),
            pltpu.VMEM((3, NLON, 128), F32),
            pltpu.VMEM((NLATD, SENT, 128), F32),
            pltpu.VMEM((NLATD, SENT, 128), F32),
            pltpu.VMEM((NLEVD, NX, SENT, 128), F32),
            pltpu.VMEM((1, 128), F32),
            pltpu.VMEM((NZ, 1, 128), F32),
            pltpu.VMEM((NX * NLEVD, NZ, 1, 128), F32),
            pltpu.VMEM((3, LEV, 40, 128), F32),
            dma((7,)), dma((2,)), dma((2,)), dma((1 + chunks,)),
            dma((chunks, NZ)), dma((chunks, NZ)), dma((NZ,)), dma((NZ,)),
            dma((NX * NLEVD,)), dma((NX * NLEVD,)),
            dma((chunks, NX * NLEVD)), dma((chunks, NX * NLEVD)),
        ],
        compiler_params=pltpu.CompilerParams(
            collective_id=0, has_side_effects=True, vmem_limit_bytes=67043328
        ),
    )(th, te, tr, ec, nc, polar_mask, wave_cutoff, level_weight, target_surface, jnp.asarray(full), jnp.asarray(real))
    return tuple(o.reshape(36, LEV, 96).transpose(1, 2, 0) for o in outs)


def solution(mesh):
    field = P("lev", "lat", None)
    return jax.shard_map(
        on_device,
        mesh=mesh,
        in_specs=(field,) * 5 + (P("lat"), P("lat"), P(), P()),
        out_specs=(P(None, "lev", "lat"),) * 3,
        check_vma=False,
    )
```

```python
import functools

import jax
import jax.numpy as jnp
import numpy as np
from jax import lax
from jax.experimental import pallas as pl
from jax.experimental.pallas import tpu as pltpu
from jax.sharding import PartitionSpec as P

MESH = pl.DeviceIdType.MESH
F32 = jnp.float32
BF16 = jnp.bfloat16

NLON, NLAT, LEV = 1152, 768, 32
ROWS = 24
LEVD = 4
NZ, NX, NY = 8, 4, 4
NLATD, NLEVD = 32, 8
RADIX, POINTS = 9, 128
SENT = 84
POLAR_BANDS = -(-(NLAT // 5) // ROWS)


def split_bf16(x):
    high = x.astype(BF16)
    return high, (x - high.astype(F32)).astype(BF16)


def tables():
    b = np.arange(POINTS)[:, None]
    full = np.zeros((4, 256, 256))
    for k1 in range(1, 5):
        angle = 2.0 * np.pi * ((b * (k1 + RADIX * np.arange(POINTS)[None, :])) % NLON) / NLON
        c, s = np.cos(angle), np.sin(angle)
        full[k1 - 1] = np.block([[c, -s], [s, c]])
    col = np.arange(POINTS)[None, :]
    wave = np.where(col <= 64, col, col - 64)
    angle = 2.0 * np.pi * ((b * wave) % POINTS) / POINTS
    real = np.where(col <= 64, np.cos(angle), np.sin(angle))

    def pair(x):
        high = x.astype(np.float32).astype(BF16)
        low = (x - high.astype(np.float64)).astype(np.float32).astype(BF16)
        return np.stack([np.asarray(high), np.asarray(low)])

    return pair(full), pair(real)


def dot3(xh, xl, th, tl, dims):
    dot = functools.partial(
        lax.dot_general, dimension_numbers=(dims, ((), ())), preferred_element_type=F32
    )
    return dot(xh, th) + dot(xl, th) + dot(xh, tl)


def lanes9(x):
    return jnp.concatenate([x] * RADIX, axis=1)


def step_kernel(
    th_hbm, te_hbm, tr_hbm, ec_hbm, nc_hbm, mask_hbm, cut_hbm, weight_hbm, target_hbm, full_hbm, real_hbm,
    thick_ref, temp_ref, tracer_ref,
    in_ref, full_ref, real_ref, s_ref, up_ref, down_ref, from_south, from_north, uh_ref, ul_ref, z_ref, t_ref,
    msg_ref, mid_ref, col_ref, part_ref, ring_sum, all_sum, r_ref,
    load_sem, halo_send, halo_recv, own_sem, zs, zr, ps, pr, rs, rr, fs, fr,
    mask_ref, cut_ref, weight_ref, target_ref,
):
    lat = lax.axis_index("lat")
    lev = lax.axis_index("lev")
    z, x = lat // NX, lax.rem(lat, NX)
    north = lax.rem(lat + 1, NLATD)
    south = lax.rem(lat + NLATD - 1, NLATD)
    polar = jnp.logical_or(lat < POLAR_BANDS, lat >= NLATD - POLAR_BANDS)

    barrier = pltpu.get_barrier_semaphore()
    for other in (north, south):
        pl.semaphore_signal(barrier, inc=1, device_id=(other, lev), device_id_type=MESH)

    def plane_peer(o):
        return z * NX + lax.rem(x + o // NLEVD, NX), lax.rem(lev + o, NLEVD)

    def greet_plane(o, carry):
        pl.semaphore_signal(barrier, inc=1, device_id=plane_peer(o), device_id_type=MESH)
        return carry

    def greet_ring(o, carry):
        peer = (lax.rem(lat + NX * o, NLATD), lev)
        pl.semaphore_signal(barrier, inc=1, device_id=peer, device_id_type=MESH)
        return carry

    lax.fori_loop(1, NZ, greet_ring, 0)
    lax.fori_loop(1, NX * NLEVD, greet_plane, 0)

    fields_hbm = (th_hbm, te_hbm, tr_hbm, nc_hbm, ec_hbm)
    loads = [pltpu.make_async_copy(fields_hbm[f], in_ref.at[f], load_sem.at[f]) for f in range(5)]
    small = ((mask_hbm, mask_ref), (cut_hbm, cut_ref), (weight_hbm, weight_ref), (target_hbm, target_ref))
    loads += [pltpu.make_async_copy(a, b, load_sem.at[7 + n]) for n, (a, b) in enumerate(small)]
    for load in loads:
        load.start()
    table_loads = (
        pltpu.make_async_copy(full_hbm, full_ref, load_sem.at[5]),
        pltpu.make_async_copy(real_hbm, real_ref, load_sem.at[6]),
    )

    @pl.when(polar)
    def _():
        for load in table_loads:
            load.start()

    for load in loads:
        load.wait()
    th_ref, te_ref, tr_ref, nc_ref, ec_ref = (in_ref.at[f] for f in range(5))
    fields = (th_ref, te_ref, tr_ref, nc_ref)
    for f in range(4):
        for l in range(LEVD):
            up_ref[pl.ds(4 * f + l, 1), :] = fields[f][l, ROWS - 1 : ROWS, :]
            if f < 3:
                down_ref[pl.ds(4 * f + l, 1), :] = fields[f][l, 0:1, :]

    def east(l, carry):
        th, te, tr = th_ref[l], te_ref[l], tr_ref[l]
        mass = ec_ref[l] * (th + pltpu.roll(th, NLON - 1, 1)) * 0.5
        temp = mass * (te + pltpu.roll(te, NLON - 1, 1)) * 0.5
        trac = mass * (tr + pltpu.roll(tr, NLON - 1, 1)) * 0.5
        s_ref[0, l] = pltpu.roll(mass, 1, 1) - mass
        s_ref[1, l] = pltpu.roll(temp, 1, 1) - temp
        s_ref[2, l] = pltpu.roll(trac, 1, 1) - trac
        return carry

    lax.fori_loop(0, LEVD, east, 0)

    pl.semaphore_wait(barrier, 2 + NZ - 1 + NX * NLEVD - 1)
    to_north = pltpu.make_async_remote_copy(
        src_ref=up_ref, dst_ref=from_south, send_sem=halo_send.at[0], recv_sem=halo_recv.at[0],
        device_id=(north, lev), device_id_type=MESH,
    )
    to_south = pltpu.make_async_remote_copy(
        src_ref=down_ref, dst_ref=from_north, send_sem=halo_send.at[1], recv_sem=halo_recv.at[1],
        device_id=(south, lev), device_id_type=MESH,
    )
    to_north.start()
    to_south.start()

    first_row = lat * ROWS
    row = (first_row + lax.broadcasted_iota(jnp.int32, (ROWS, 128), 0)).astype(F32)
    center = lanes9(jnp.sin((row + 0.5) * np.float32(np.pi) / NLAT))
    face = lanes9(jnp.sin((row + 1.0) * np.float32(np.pi) / NLAT))
    face_below = face_below_row(first_row)
    inverse_center = 1.0 / center
    row_in = lax.broadcasted_iota(jnp.int32, (ROWS, NLON), 0)

    to_north.wait()
    to_south.wait()

    for l in range(LEVD):
        th, te, tr = th_ref[l], te_ref[l], tr_ref[l]

        def above(v, f):
            edge = from_north[4 * f + l : 4 * f + l + 1, :]
            edge = jnp.where(lat == NLATD - 1, 0.0, edge)
            return jnp.where(row_in == ROWS - 1, edge, pltpu.roll(v, ROWS - 1, 0))

        def south_row(f):
            return from_south[4 * f + l : 4 * f + l + 1, :]

        mass = nc_ref[l] * (th + above(th, 0)) * 0.5 * face
        temp = mass * (te + above(te, 1)) * 0.5
        trac = mass * (tr + above(tr, 2)) * 0.5
        mass_s = south_row(3) * (south_row(0) + th[0:1]) * 0.5 * face_below
        temp_s = mass_s * (south_row(1) + te[0:1]) * 0.5
        trac_s = mass_s * (south_row(2) + tr[0:1]) * 0.5
        for f, (flux, below) in enumerate(((mass, mass_s), (temp, temp_s), (trac, trac_s))):
            lower = jnp.where(row_in == 0, below, pltpu.roll(flux, 1, 0))
            s_ref[f, l] = s_ref[f, l] - (flux - lower) * inverse_center

    @pl.when(polar)
    def _():
        for load in table_loads:
            load.wait()
        polar_filter(mask_ref, cut_ref, full_ref, real_ref, s_ref, uh_ref, ul_ref, z_ref)

    def update(l, total):
        th, te, tr = th_ref[l], te_ref[l], tr_ref[l]
        mass = s_ref[0, l]
        inverse = 1.0 / th
        new_th = th + mass
        s_ref[0, l] = new_th
        s_ref[1, l] = te + (s_ref[1, l] - te * mass) * inverse
        s_ref[2, l] = tr + (s_ref[2, l] - tr * mass) * inverse
        weighted = new_th * center
        for a in range(RADIX):
            part = weighted[:, 128 * a : 128 * a + 128]
            total = total + (part[0:8] + part[8:16] + part[16:24])
        return total

    total = lax.fori_loop(0, LEVD, update, jnp.zeros((8, 128), F32))
    total = jnp.sum(total, axis=0, keepdims=True)
    part_ref[...] = total
    ring_sum[z] = total

    flat = s_ref.reshape(3 * LEVD * ROWS, NLON)
    for a in range(RADIX):
        at = pl.ds(128 * a, 128)
        one = jnp.concatenate([flat[0:120, at], flat[264:272, at]], axis=0)
        two = jnp.concatenate([flat[120:240, at], flat[272:280, at]], axis=0)
        last = jnp.concatenate([flat[240:264, at], flat[280:288, at]], axis=0)
        t_ref[0, at, :] = one.T
        t_ref[1, at, :] = two.T
        t_ref[2, at, :] = jnp.concatenate([last] * 4, axis=0).T

    sub = lax.broadcasted_iota(jnp.int32, (8, 128), 0)
    lane = lax.broadcasted_iota(jnp.int32, (8, 128), 1)

    def pack(p, carry):
        base = 72 * p

        def tile(q, j, n=1):
            return t_ref[q, pl.ds(pl.multiple_of(base + 8 * j, 8), 8 * n), :]

        def fours(u):
            return jnp.where(
                lane < 64, jnp.where(lane < 32, u[0], u[1]), jnp.where(lane < 96, u[2], u[3])
            )

        for q in range(2):
            for j in range(4):
                at = pl.ds(TILE_ROW[j] + TILE_STEP[j] * q, 8)
                msg_ref[2 * p, at, :] = tile(q, j)
                msg_ref[2 * p + 1, at, :] = tile(q, 5 + j)
        t0, t1, t2 = tile(0, 4), tile(1, 4), tile(2, 4)
        msg_ref[2 * p, 72:80, :] = jnp.where(sub < 4, t0, pltpu.roll(t1, 4, 0))
        msg_ref[2 * p + 1, 72:80, :] = jnp.where(sub < 4, pltpu.roll(t0, 4, 0), t1)
        msg_ref[2 * p, 32:40, :] = fours([tile(2, j) for j in range(4)])
        msg_ref[2 * p + 1, 32:40, :] = fours([tile(2, j) for j in range(5, 9)])
        msg_ref[2 * p, 80:84, :] = t2[0:4]
        msg_ref[2 * p + 1, 80:84, :] = pltpu.roll(t2, 4, 0)[0:4]
        return carry

    lax.fori_loop(0, NLATD // 2, pack, 0)

    def ring_part(o):
        return pltpu.make_async_remote_copy(
            src_ref=part_ref, dst_ref=ring_sum.at[z], send_sem=ps.at[0], recv_sem=pr.at[0],
            device_id=(lax.rem(lat + NX * o, NLATD), lev), device_id_type=MESH,
        )

    def plane_part(o):
        return pltpu.make_async_remote_copy(
            src_ref=ring_sum, dst_ref=all_sum.at[x * NLEVD + lev], send_sem=rs.at[0], recv_sem=rr.at[0],
            device_id=plane_peer(o), device_id_type=MESH,
        )

    def all_of(ref, sem):
        pltpu.make_async_copy(ref, ref, sem).wait()

    def each(count, action, start=0):
        def body(o, carry):
            action(o)
            return carry

        lax.fori_loop(start, count, body, 0)

    each(NZ, lambda o: ring_part(o).start(), 1)

    def distance(k):
        return jnp.where(lax.rem(k, 2) == 1, (k + 1) // 2, lax.rem(NZ - k // 2, NZ))

    def along_z(chunk, k):
        to = lax.rem(z + distance(k), NZ)
        first, count = CHUNKS[chunk]
        return pltpu.make_async_remote_copy(
            src_ref=msg_ref.at[pl.ds(NX * to, NX), pl.ds(first, count)],
            dst_ref=mid_ref.at[pl.ds(NX * z, NX), pl.ds(first, count)],
            send_sem=zs.at[chunk], recv_sem=zr.at[chunk, k],
            device_id=(to * NX + x, lev), device_id_type=MESH,
        )

    for chunk in range(len(CHUNKS)):
        each(NZ, lambda k: along_z(chunk, k).start(), 1)
    mine = pltpu.make_async_copy(
        msg_ref.at[pl.ds(NX * z, NX)], mid_ref.at[pl.ds(NX * z, NX)], own_sem.at[0]
    )
    mine.start()

    all_of(ring_sum.at[pl.ds(0, NZ - 1)], pr.at[0])
    each(NX * NLEVD, lambda o: plane_part(o).start(), 1)
    mine.wait()

    def onward(chunk, source, to_x):
        first, count = CHUNKS[chunk]
        piece = mid_ref.at[NX * source + to_x, pl.ds(first, count)]
        place = col_ref.at[lev, x, pl.ds(first, count)]
        away = pltpu.make_async_remote_copy(
            src_ref=piece, dst_ref=place, send_sem=fs.at[chunk], recv_sem=fr.at[chunk],
            device_id=(z * NX + to_x, source), device_id_type=MESH,
        )
        stay = pltpu.make_async_copy(piece, place, fr.at[chunk])
        return away, stay

    def forward(chunk, k):
        source = lax.rem(z + NZ - distance(k), NZ)

        @pl.when(k > 0)
        def _():
            along_z(chunk, k).wait_recv()

        for dx in ACROSS:
            away, stay = onward(chunk, source, lax.rem(x + dx, NX))
            if dx == 0:
                pl.when(source != lev)(away.start)
                pl.when(source == lev)(stay.start)
            else:
                away.start()

    def arrived(chunk):
        first, count = CHUNKS[chunk]
        all_of(mid_ref.at[:, pl.ds(first, count)], fr.at[chunk])

    remap = Remap(lat, lane, col_ref, r_ref, weight_ref, target_ref, thick_ref, temp_ref, tracer_ref)

    each(NZ, lambda k: forward(0, k))
    each(4, lambda k: forward(1, k))
    all_of(all_sum.at[pl.ds(0, NX * NLEVD - 1)], rr.at[0])
    all_sum[x * NLEVD + lev] = ring_sum[...]
    remap.set_scale(all_sum)
    arrived(0)
    remap.unpack((0, 1))

    def early(j):
        remap.tile(j)
        forward(1, 4 + 2 * j)
        forward(1, 5 + 2 * j)

    each(2, early)
    each(5, lambda k: forward(2, k))
    arrived(1)
    remap.unpack((2, 4))
    remap.tile(2)
    each(NZ, lambda k: forward(2, k), 5)
    remap.half_tile()
    all_of(ring_sum.at[pl.ds(0, NZ - 1)], ps.at[0])
    all_of(all_sum.at[pl.ds(0, NX * NLEVD - 1)], rs.at[0])
    for chunk, (first, count) in enumerate(CHUNKS):
        all_of(mid_ref.at[pl.ds(0, NX * (NZ - 1)), pl.ds(first, count)], zs.at[chunk])
        all_of(mid_ref.at[pl.ds(0, NX * NLEVD - 1), pl.ds(first, count)], fs.at[chunk])
    arrived(2)
    remap.unpack((3,))
    remap.tile(3)


def face_below_row(first_row):
    row = lax.broadcasted_iota(jnp.int32, (8, 128), 0) * 0 + first_row
    below = jnp.sin(row.astype(F32) * np.float32(np.pi) / NLAT)
    return lanes9(below[0:1])


def polar_filter(mask_ref, cut_ref, full_ref, real_ref, s_ref, uh_ref, ul_ref, z_ref):
    rows = 3 * LEVD * ROWS
    flat = s_ref.reshape(rows, NLON)
    cos9 = [[np.float32(np.cos(2 * np.pi * a * k / 9)) for k in range(5)] for a in range(5)]
    sin9 = [[np.float32(np.sin(2 * np.pi * a * k / 9)) for k in range(5)] for a in range(5)]

    def forward(r, carry):
        at = pl.ds(pl.multiple_of(16 * r, 16), 16)
        v = [flat[at, 128 * a : 128 * a + 128] for a in range(RADIX)]
        even = [v[a] + v[9 - a] for a in range(1, 5)]
        odd = [v[a] - v[9 - a] for a in range(1, 5)]

        def put(slot, x):
            high, low = split_bf16(x)
            uh_ref[at, 128 * slot : 128 * slot + 128] = high
            ul_ref[at, 128 * slot : 128 * slot + 128] = low

        put(8, v[0] + ((even[0] + even[1]) + (even[2] + even[3])))
        for k in range(1, 5):
            put(2 * k - 2, v[0] + sum(even[a - 1] * cos9[a][k] for a in range(1, 5)))
            put(2 * k - 1, -sum(odd[a - 1] * sin9[a][k] for a in range(1, 5)))
        return carry

    lax.fori_loop(0, rows // 16, forward, 0)

    row24 = lax.broadcasted_iota(jnp.int32, (ROWS, 128), 0)
    lane24 = lax.broadcasted_iota(jnp.int32, (ROWS, 128), 1)
    cuts = jnp.full((ROWS, 128), 10000, jnp.int32)
    for r in range(ROWS):
        cuts = jnp.where(row24 == r, jnp.where(mask_ref[r] > 0, cut_ref[r], 10000), cuts)

    for k in range(1, 5):
        wave = k + RADIX * lane24
        keep = (jnp.minimum(wave, NLON - wave) >= cuts).astype(F32)
        keep = jnp.concatenate([jnp.concatenate([keep, keep], axis=1)] * 12, axis=0)
        at = pl.ds(256 * (k - 1), 256)
        tables_k = full_ref[0, k - 1], full_ref[1, k - 1]
        x = dot3(uh_ref[:, at], ul_ref[:, at], *tables_k, ((1,), (0,)))
        xh, xl = split_bf16(x * keep)
        z_ref[:, at] = dot3(xh, xl, *tables_k, ((1,), (1,)))
    wave = RADIX * jnp.where(lane24 <= 64, lane24, lane24 - 64)
    weight = jnp.where(jnp.logical_or(lane24 == 0, lane24 == 64), 1.0, 2.0)
    keep = jnp.concatenate([jnp.where(wave >= cuts, weight, 0.0)] * 12, axis=0)
    x = dot3(uh_ref[:, 1024:1152], ul_ref[:, 1024:1152], real_ref[0], real_ref[1], ((1,), (0,)))
    xh, xl = split_bf16(x * keep)
    z_ref[:, 1024:1152] = dot3(xh, xl, real_ref[0], real_ref[1], ((1,), (1,)))

    def backward(r, carry):
        at = pl.ds(pl.multiple_of(8 * r, 8), 8)
        z0 = z_ref[at, 1024:1152] * np.float32(1.0 / NLON)
        zr = [z_ref[at, 256 * k : 256 * k + 128] * np.float32(2.0 / NLON) for k in range(4)]
        zi = [z_ref[at, 256 * k + 128 : 256 * k + 256] * np.float32(2.0 / NLON) for k in range(4)]
        flat[at, 0:128] = flat[at, 0:128] - (z0 + ((zr[0] + zr[1]) + (zr[2] + zr[3])))
        for a in range(1, 5):
            even = z0 + sum(zr[k - 1] * cos9[a][k] for k in range(1, 5))
            odd = sum(zi[k - 1] * sin9[a][k] for k in range(1, 5))
            lo, hi = pl.ds(128 * a, 128), pl.ds(128 * (9 - a), 128)
            flat[at, lo] = flat[at, lo] - (even - odd)
            flat[at, hi] = flat[at, hi] - (even + odd)
        return carry

    lax.fori_loop(0, rows // 8, backward, 0)


ACROSS = (0, 1, 3, 2)
CHUNKS = ((0, 40), (56, 28), (40, 16))
TILE_ROW = (0, 8, 56, 40)
TILE_STEP = (16, 16, 8, 8)


class Remap:
    def __init__(self, lat, lane, col_ref, r_ref, weight_ref, target_ref, thick_ref, temp_ref, tracer_ref):
        self.odd = lax.rem(lat, 2)
        self.lane = lane
        self.col_ref, self.r_ref, self.target_ref = col_ref, r_ref, target_ref
        self.outs = thick_ref, temp_ref, tracer_ref
        self.weights = [weight_ref[k] for k in range(LEV)]
        whole = self.weights[0]
        for k in range(1, LEV):
            whole = whole + self.weights[k]
        self.whole = whole

    def set_scale(self, all_sum):
        area = float(np.sum(np.sin((np.arange(NLAT) + 0.5) * np.pi / NLAT)))
        total = jnp.sum(all_sum[...].reshape(NX * NLEVD * NZ, 128), axis=0, keepdims=True)
        total = jnp.sum(total, axis=1, keepdims=True)
        self.scale = jnp.broadcast_to(self.target_ref[0] * (NLON * area) / total, (8, 128))

    def unpack(self, tiles):
        lane, col_ref, r_ref = self.lane, self.col_ref, self.r_ref

        def merge(parts):
            return jnp.where(
                lane < 48, jnp.where(lane < 24, parts[0], parts[1]), jnp.where(lane < 72, parts[2], parts[3])
            )

        def move(v, source, target):
            amount = (target - source) % 128
            return v if amount == 0 else pltpu.roll(v, amount, 1)

        phase = jnp.where(
            lane >= 72, lane - 72, jnp.where(lane >= 48, lane - 48, jnp.where(lane >= 24, lane - 24, lane))
        )

        def body(g, carry):
            for j in tiles:
                if j < 4:
                    one = [col_ref[g, x, pl.ds(TILE_ROW[j], 8), :] for x in range(4)]
                    two = [col_ref[g, x, pl.ds(TILE_ROW[j] + TILE_STEP[j], 8), :] for x in range(4)]
                    last = [col_ref[g, x, 32:40, :] for x in range(4)]
                    lane0 = 32 * j
                else:
                    one = [col_ref[g, x, 72:80, :] for x in range(4)]
                    two = [pltpu.roll(v, 4, 0) for v in one]
                    last = [col_ref[g, x, 80:84, :] for x in range(4)]
                    last = [jnp.concatenate([v, v], axis=0) for v in last]
                    lane0 = 0

                def put(fl, v):
                    r_ref[fl // 4, g * 4 + fl % 4, 8 * j : 8 * j + 8, :] = v

                for n in range(5):
                    put(n, merge([move(one[x], 24 * n, 24 * x) for x in range(4)]))
                    put(5 + n, merge([move(two[x], 24 * n, 24 * x) for x in range(4)]))
                put(10, merge([move(last[x], lane0, 24 * x) for x in range(4)]))
                a = merge([move(one[x], 120, 24 * x) for x in range(4)])
                b = merge([move(two[x], 120, 24 * x + 8) for x in range(4)])
                c = merge([move(last[x], lane0 + 24, 24 * x + 16) for x in range(4)])
                put(11, jnp.where(phase < 8, a, jnp.where(phase < 16, b, c)))
            return carry

        lax.fori_loop(0, NLEVD, body, 0)

    def tile(self, j):
        self.columns(j, 8, 8 * j + 4 * self.odd)

    def half_tile(self):
        self.columns(4, 4, 32 - 32 * self.odd)

    def columns(self, j, count, lon0):
        weights, r_ref = self.weights, self.r_ref
        thick_ref, temp_ref, tracer_ref = self.outs
        at = pl.ds(pl.multiple_of(8 * j, 8), 8)
        surface = r_ref[0, 0, at, :]
        for m in range(1, LEV):
            surface = surface + r_ref[0, m, at, :]
        unit = surface / jnp.full((8, 128), self.whole)
        previous = (jnp.zeros((8, 128), F32), jnp.zeros((8, 128), F32))
        running = None
        for k0 in range(0, LEV, 8):
            bounds = []
            for k in range(k0, k0 + 8):
                running = weights[k] if running is None else running + weights[k]
                bounds.append(unit * running)
            temps = [jnp.zeros((8, 128), F32)] * 8
            tracs = [jnp.zeros((8, 128), F32)] * 8
            top = jnp.zeros((8, 128), F32)
            for m in range(LEV):
                th = r_ref[0, m, at, :]
                te = r_ref[1, m, at, :]
                tr = r_ref[2, m, at, :]
                for n in range(8):
                    part = jnp.minimum(jnp.maximum(bounds[n] - top, 0.0), th)
                    temps[n] = temps[n] + te * part
                    tracs[n] = tracs[n] + tr * part
                top = top + th
            for n in range(8):
                k = k0 + n
                target = unit * weights[k]
                inverse = 1.0 / target
                rows = pl.ds(lon0 * LEV + k, count, stride=LEV)
                thick_ref[rows, :] = (target * self.scale)[0:count, 0:96]
                temp_ref[rows, :] = ((temps[n] - previous[0]) * inverse)[0:count, 0:96]
                tracer_ref[rows, :] = ((tracs[n] - previous[1]) * inverse)[0:count, 0:96]
                previous = (temps[n], tracs[n])


def on_device(th, te, tr, ec, nc, polar_mask, wave_cutoff, level_weight, target_surface):
    vmem = pl.BlockSpec(memory_space=pltpu.VMEM)
    hbm = pl.BlockSpec(memory_space=pl.ANY)
    full, real = tables()
    dma = pltpu.SemaphoreType.DMA
    chunks = len(CHUNKS)
    outs = pl.pallas_call(
        step_kernel,
        name="step",
        out_shape=tuple(jax.ShapeDtypeStruct((36 * LEV, 96), F32) for _ in range(3)),
        in_specs=[hbm] * 11,
        out_specs=(vmem, vmem, vmem),
        scratch_shapes=[
            pltpu.VMEM((5, LEVD, ROWS, NLON), F32),
            pltpu.VMEM(full.shape, BF16),
            pltpu.VMEM(real.shape, BF16),
            pltpu.VMEM((3, LEVD, ROWS, NLON), F32),
            pltpu.VMEM((16, NLON), F32),
            pltpu.VMEM((12, NLON), F32),
            pltpu.VMEM((16, NLON), F32),
            pltpu.VMEM((12, NLON), F32),
            pltpu.VMEM((288, NLON), BF16),
            pltpu.VMEM((288, NLON), BF16),
            pltpu.VMEM((288, NLON), F32),
            pltpu.VMEM((3, NLON, 128), F32),
            pltpu.VMEM((NLATD, SENT, 128), F32),
            pltpu.VMEM((NLATD, SENT, 128), F32),
            pltpu.VMEM((NLEVD, NX, SENT, 128), F32),
            pltpu.VMEM((1, 128), F32),
            pltpu.VMEM((NZ, 1, 128), F32),
            pltpu.VMEM((NX * NLEVD, NZ, 1, 128), F32),
            pltpu.VMEM((3, LEV, 40, 128), F32),
            dma((11,)), dma((2,)), dma((2,)), dma((1,)),
            dma((chunks,)), dma((chunks, NZ)), dma((1,)), dma((1,)), dma((1,)), dma((1,)),
            dma((chunks,)), dma((chunks,)),
            pltpu.SMEM((ROWS,), jnp.int32), pltpu.SMEM((ROWS,), jnp.int32),
            pltpu.SMEM((LEV,), F32), pltpu.SMEM((1,), F32),
        ],
        compiler_params=pltpu.CompilerParams(
            collective_id=0, has_side_effects=True, vmem_limit_bytes=67043328
        ),
    )(th, te, tr, ec, nc, polar_mask, wave_cutoff, level_weight, target_surface, jnp.asarray(full), jnp.asarray(real))
    return tuple(o.reshape(36, LEV, 96).transpose(1, 2, 0) for o in outs)


def solution(mesh):
    field = P("lev", "lat", None)
    return jax.shard_map(
        on_device,
        mesh=mesh,
        in_specs=(field,) * 5 + (P("lat"), P("lat"), P(), P()),
        out_specs=(P(None, "lev", "lat"),) * 3,
        check_vma=False,
    )
```

```python
import functools

import jax
import jax.numpy as jnp
import numpy as np
from jax import lax
from jax.experimental import pallas as pl
from jax.experimental.pallas import tpu as pltpu
from jax.sharding import PartitionSpec as P

MESH = pl.DeviceIdType.MESH
F32 = jnp.float32
BF16 = jnp.bfloat16

NLON, NLAT, LEV = 1152, 768, 32
ROWS = 24
LEVD = 4
NZ, NX, NY = 8, 4, 4
NLATD, NLEVD = 32, 8
RADIX, POINTS = 9, 128
SENT = 84
POLAR_BANDS = -(-(NLAT // 5) // ROWS)


def split_bf16(x):
    high = x.astype(BF16)
    return high, (x - high.astype(F32)).astype(BF16)


def tables():
    b = np.arange(POINTS)[:, None]
    full = np.zeros((4, 256, 256))
    for k1 in range(1, 5):
        angle = 2.0 * np.pi * ((b * (k1 + RADIX * np.arange(POINTS)[None, :])) % NLON) / NLON
        c, s = np.cos(angle), np.sin(angle)
        full[k1 - 1] = np.block([[c, -s], [s, c]])
    col = np.arange(POINTS)[None, :]
    wave = np.where(col <= 64, col, col - 64)
    angle = 2.0 * np.pi * ((b * wave) % POINTS) / POINTS
    real = np.where(col <= 64, np.cos(angle), np.sin(angle))

    def pair(x):
        high = x.astype(np.float32).astype(BF16)
        low = (x - high.astype(np.float64)).astype(np.float32).astype(BF16)
        return np.stack([np.asarray(high), np.asarray(low)])

    return pair(full), pair(real)


def dot3(xh, xl, th, tl, dims):
    dot = functools.partial(
        lax.dot_general, dimension_numbers=(dims, ((), ())), preferred_element_type=F32
    )
    rows = xh.shape[0]
    both = dot(jnp.concatenate([xh, xl], axis=0), th)
    return both[:rows] + both[rows:] + dot(xh, tl)


def lanes9(x):
    return jnp.concatenate([x] * RADIX, axis=1)


def step_kernel(
    th_hbm, te_hbm, tr_hbm, ec_hbm, nc_hbm, mask_hbm, cut_hbm, weight_hbm, target_hbm, full_hbm, real_hbm,
    thick_hbm, temp_hbm, tracer_hbm, late_hbm, quarter_hbm, scale_hbm,
    thick_ref, temp_ref, tracer_ref, scale_ref,
    in_ref, full_ref, real_ref, s_ref, up_ref, down_ref, from_south, from_north, edge_ref, uh_ref, ul_ref, z_ref, t_ref,
    msg_ref, mid_ref, col_ref, part_ref, ring_sum, all_sum, r_ref,
    load_sem, halo_send, halo_recv, own_sem, zs, zr, ps, pr, rs, rr, fs, fr,
    mask_ref, cut_ref, weight_ref, target_ref, out_sem,
):
    lat = lax.axis_index("lat")
    lev = lax.axis_index("lev")
    z, x = lat // NX, lax.rem(lat, NX)
    north = lax.rem(lat + 1, NLATD)
    south = lax.rem(lat + NLATD - 1, NLATD)
    polar = jnp.logical_or(lat < POLAR_BANDS, lat >= NLATD - POLAR_BANDS)

    barrier = pltpu.get_barrier_semaphore()
    for other in (north, south):
        pl.semaphore_signal(barrier, inc=1, device_id=(other, lev), device_id_type=MESH)

    def plane_peer(o):
        return z * NX + lax.rem(x + o // NLEVD, NX), lax.rem(lev + o, NLEVD)

    def greet_plane(o, carry):
        pl.semaphore_signal(barrier, inc=1, device_id=plane_peer(o), device_id_type=MESH)
        return carry

    def greet_ring(o, carry):
        peer = (lax.rem(lat + NX * o, NLATD), lev)
        pl.semaphore_signal(barrier, inc=1, device_id=peer, device_id_type=MESH)
        return carry

    lax.fori_loop(1, NZ, greet_ring, 0)
    lax.fori_loop(1, NX * NLEVD, greet_plane, 0)

    fields_hbm = (th_hbm, te_hbm, tr_hbm, nc_hbm, ec_hbm)
    loads = [pltpu.make_async_copy(fields_hbm[f], in_ref.at[f], load_sem.at[f]) for f in range(5)]
    small = ((mask_hbm, mask_ref), (cut_hbm, cut_ref), (weight_hbm, weight_ref), (target_hbm, target_ref))
    loads += [pltpu.make_async_copy(a, b, load_sem.at[7 + n]) for n, (a, b) in enumerate(small)]
    for load in loads:
        load.start()
    table_loads = (
        pltpu.make_async_copy(full_hbm, full_ref, load_sem.at[5]),
        pltpu.make_async_copy(real_hbm, real_ref, load_sem.at[6]),
    )

    @pl.when(polar)
    def _():
        for load in table_loads:
            load.start()

    for load in loads:
        load.wait()
    th_ref, te_ref, tr_ref, nc_ref, ec_ref = (in_ref.at[f] for f in range(5))
    fields = (th_ref, te_ref, tr_ref, nc_ref)
    for f in range(4):
        for l in range(LEVD):
            up_ref[pl.ds(4 * f + l, 1), :] = fields[f][l, ROWS - 1 : ROWS, :]
            if f < 3:
                down_ref[pl.ds(4 * f + l, 1), :] = fields[f][l, 0:1, :]

    def east(l, carry):
        th, te, tr = th_ref[l], te_ref[l], tr_ref[l]
        mass = ec_ref[l] * (th + pltpu.roll(th, NLON - 1, 1)) * 0.5
        temp = mass * (te + pltpu.roll(te, NLON - 1, 1)) * 0.5
        trac = mass * (tr + pltpu.roll(tr, NLON - 1, 1)) * 0.5
        s_ref[0, l] = pltpu.roll(mass, 1, 1) - mass
        s_ref[1, l] = pltpu.roll(temp, 1, 1) - temp
        s_ref[2, l] = pltpu.roll(trac, 1, 1) - trac
        return carry

    lax.fori_loop(0, LEVD, east, 0)

    first_row = lat * ROWS
    row = (first_row + lax.broadcasted_iota(jnp.int32, (ROWS, 128), 0)).astype(F32)
    center = lanes9(jnp.sin((row + 0.5) * np.float32(np.pi) / NLAT))
    face = lanes9(jnp.sin((row + 1.0) * np.float32(np.pi) / NLAT))
    inverse_center = 1.0 / center
    row_in = lax.broadcasted_iota(jnp.int32, (ROWS, NLON), 0)

    def inner(l, carry):
        th, te, tr = th_ref[l], te_ref[l], tr_ref[l]

        def above(v):
            return pltpu.roll(v, ROWS - 1, 0)

        mass = nc_ref[l] * (th + above(th)) * 0.5 * face
        mass = jnp.where(row_in == ROWS - 1, 0.0, mass)
        temp = mass * (te + above(te)) * 0.5
        trac = mass * (tr + above(tr)) * 0.5
        for f, flux in enumerate((mass, temp, trac)):
            s_ref[f, l] = s_ref[f, l] - (flux - pltpu.roll(flux, 1, 0)) * inverse_center
        return carry

    lax.fori_loop(0, LEVD, inner, 0)
    flat = s_ref.reshape(3 * LEVD * ROWS, NLON)
    scratch = full_ref, real_ref, uh_ref, ul_ref, z_ref

    @pl.when(polar)
    def _():
        for load in table_loads:
            load.wait()
        cuts = row_cuts(mask_ref, cut_ref)
        polar_filter(flat, 3 * LEVD * ROWS, jnp.concatenate([cuts] * (3 * LEVD), axis=0), *scratch)

    pl.semaphore_wait(barrier, 2 + NZ - 1 + NX * NLEVD - 1)
    to_north = pltpu.make_async_remote_copy(
        src_ref=up_ref, dst_ref=from_south, send_sem=halo_send.at[0], recv_sem=halo_recv.at[0],
        device_id=(north, lev), device_id_type=MESH,
    )
    to_south = pltpu.make_async_remote_copy(
        src_ref=down_ref, dst_ref=from_north, send_sem=halo_send.at[1], recv_sem=halo_recv.at[1],
        device_id=(south, lev), device_id_type=MESH,
    )
    has_north, has_south = lat < NLATD - 1, lat > 0
    pl.when(has_north)(to_north.start)
    pl.when(has_south)(to_south.start)
    pl.when(has_south)(to_north.wait_recv)
    pl.when(has_north)(to_south.wait_recv)

    def rows_of(ref, f):
        return ref[4 * f : 4 * f + 4, :]

    def beyond(ref, f, there):
        return jnp.where(there, rows_of(ref, f), 0.0)

    def faces(courant, own, other, face_row):
        mass = courant * (own[0] + other[0]) * 0.5 * face_row
        return mass, mass * (own[1] + other[1]) * 0.5, mass * (own[2] + other[2]) * 0.5

    top = faces(
        rows_of(up_ref, 3), [rows_of(up_ref, f) for f in range(3)],
        [beyond(from_north, f, has_north) for f in range(3)], face[ROWS - 1 : ROWS],
    )
    bottom = faces(
        beyond(from_south, 3, has_south), [beyond(from_south, f, has_south) for f in range(3)],
        [rows_of(down_ref, f) for f in range(3)], face_below_row(first_row),
    )
    for f in range(3):
        edge_ref[4 * f : 4 * f + 4, :] = -top[f] * inverse_center[ROWS - 1 : ROWS]
        edge_ref[12 + 4 * f : 16 + 4 * f, :] = bottom[f] * inverse_center[0:1]
    edge_ref[24:32, :] = jnp.zeros((8, NLON), F32)

    @pl.when(polar)
    def _():
        cuts = row_cuts(mask_ref, cut_ref)
        edge_row = lax.broadcasted_iota(jnp.int32, (32, 128), 0)
        cuts = jnp.where(edge_row < 12, cuts[ROWS - 1 : ROWS], cuts[0:1])
        polar_filter(edge_ref, 32, cuts, *scratch)

    for f in range(3):
        for l in range(LEVD):
            n = 4 * f + l
            s_ref[f, l, ROWS - 1 : ROWS, :] = s_ref[f, l, ROWS - 1 : ROWS, :] + edge_ref[n : n + 1, :]
            s_ref[f, l, 0:1, :] = s_ref[f, l, 0:1, :] + edge_ref[12 + n : 13 + n, :]
    pl.when(has_north)(to_north.wait_send)
    pl.when(has_south)(to_south.wait_send)

    def update(l, total):
        th, te, tr = th_ref[l], te_ref[l], tr_ref[l]
        mass = s_ref[0, l]
        inverse = 1.0 / th
        new_th = th + mass
        s_ref[0, l] = new_th
        s_ref[1, l] = te + (s_ref[1, l] - te * mass) * inverse
        s_ref[2, l] = tr + (s_ref[2, l] - tr * mass) * inverse
        weighted = new_th * center
        for a in range(RADIX):
            part = weighted[:, 128 * a : 128 * a + 128]
            total = total + (part[0:8] + part[8:16] + part[16:24])
        return total

    total = lax.fori_loop(0, LEVD, update, jnp.zeros((8, 128), F32))
    total = jnp.sum(total, axis=0, keepdims=True)
    part_ref[...] = total
    ring_sum[z] = total

    for a in range(RADIX):
        at = pl.ds(128 * a, 128)
        one = jnp.concatenate([flat[0:120, at], flat[264:272, at]], axis=0)
        two = jnp.concatenate([flat[120:240, at], flat[272:280, at]], axis=0)
        last = jnp.concatenate([flat[240:264, at], flat[280:288, at]], axis=0)
        t_ref[0, at, :] = one.T
        t_ref[1, at, :] = two.T
        t_ref[2, at, :] = jnp.concatenate([last] * 4, axis=0).T

    sub = lax.broadcasted_iota(jnp.int32, (8, 128), 0)
    lane = lax.broadcasted_iota(jnp.int32, (8, 128), 1)

    def pack(p, carry):
        base = 72 * p

        def tile(q, j, n=1):
            return t_ref[q, pl.ds(pl.multiple_of(base + 8 * j, 8), 8 * n), :]

        def fours(u):
            return jnp.where(
                lane < 64, jnp.where(lane < 32, u[0], u[1]), jnp.where(lane < 96, u[2], u[3])
            )

        for q in range(2):
            for j in range(4):
                at = pl.ds(TILE_ROW[j] + TILE_STEP[j] * q, 8)
                msg_ref[2 * p, at, :] = tile(q, j)
                msg_ref[2 * p + 1, at, :] = tile(q, 5 + j)
        t0, t1, t2 = tile(0, 4), tile(1, 4), tile(2, 4)
        msg_ref[2 * p, 72:80, :] = jnp.where(sub < 4, t0, pltpu.roll(t1, 4, 0))
        msg_ref[2 * p + 1, 72:80, :] = jnp.where(sub < 4, pltpu.roll(t0, 4, 0), t1)
        msg_ref[2 * p, 32:40, :] = fours([tile(2, j) for j in range(4)])
        msg_ref[2 * p + 1, 32:40, :] = fours([tile(2, j) for j in range(5, 9)])
        msg_ref[2 * p, 80:84, :] = t2[0:4]
        msg_ref[2 * p + 1, 80:84, :] = pltpu.roll(t2, 4, 0)[0:4]
        return carry

    lax.fori_loop(0, NLATD // 2, pack, 0)

    def ring_part(o):
        return pltpu.make_async_remote_copy(
            src_ref=part_ref, dst_ref=ring_sum.at[z], send_sem=ps.at[0], recv_sem=pr.at[0],
            device_id=(lax.rem(lat + NX * o, NLATD), lev), device_id_type=MESH,
        )

    def plane_part(o):
        return pltpu.make_async_remote_copy(
            src_ref=ring_sum, dst_ref=all_sum.at[x * NLEVD + lev], send_sem=rs.at[0], recv_sem=rr.at[0],
            device_id=plane_peer(o), device_id_type=MESH,
        )

    def all_of(ref, sem):
        pltpu.make_async_copy(ref, ref, sem).wait()

    def each(count, action, start=0):
        def body(o, carry):
            action(o)
            return carry

        lax.fori_loop(start, count, body, 0)

    each(NZ, lambda o: ring_part(o).start(), 1)

    def distance(k):
        return jnp.where(lax.rem(k, 2) == 1, (k + 1) // 2, lax.rem(NZ - k // 2, NZ))

    def along_z(chunk, k):
        to = lax.rem(z + distance(k), NZ)
        first, count = CHUNKS[chunk]
        return pltpu.make_async_remote_copy(
            src_ref=msg_ref.at[pl.ds(NX * to, NX), pl.ds(first, count)],
            dst_ref=mid_ref.at[pl.ds(NX * z, NX), pl.ds(first, count)],
            send_sem=zs.at[chunk], recv_sem=zr.at[chunk, k],
            device_id=(to * NX + x, lev), device_id_type=MESH,
        )

    for chunk in range(len(CHUNKS)):
        each(NZ, lambda k: along_z(chunk, k).start(), 1)
    mine = pltpu.make_async_copy(
        msg_ref.at[pl.ds(NX * z, NX)], mid_ref.at[pl.ds(NX * z, NX)], own_sem.at[0]
    )
    mine.start()

    all_of(ring_sum.at[pl.ds(0, NZ - 1)], pr.at[0])
    each(NX * NLEVD, lambda o: plane_part(o).start(), 1)
    mine.wait()

    def onward(chunk, source, to_x):
        first, count = CHUNKS[chunk]
        piece = mid_ref.at[NX * source + to_x, pl.ds(first, count)]
        place = late_hbm.at[lev, x] if chunk == LAST else col_ref.at[lev, x, pl.ds(first, count)]
        away = pltpu.make_async_remote_copy(
            src_ref=piece, dst_ref=place, send_sem=fs.at[chunk], recv_sem=fr.at[chunk],
            device_id=(z * NX + to_x, source), device_id_type=MESH,
        )
        stay = pltpu.make_async_copy(piece, place, fr.at[chunk])
        return away, stay

    def forward(chunk, k):
        source = lax.rem(z + NZ - distance(k), NZ)

        @pl.when(k > 0)
        def _():
            along_z(chunk, k).wait_recv()

        for dx in ACROSS:
            away, stay = onward(chunk, source, lax.rem(x + dx, NX))
            if dx == 0:
                pl.when(source != lev)(away.start)
                pl.when(source == lev)(stay.start)
            else:
                away.start()

    def arrived(chunk):
        first, count = CHUNKS[chunk]
        all_of(mid_ref.at[:, pl.ds(first, count)], fr.at[chunk])

    remap = Remap(lat, lane, r_ref, weight_ref, thick_ref, temp_ref, tracer_ref)

    each(NZ, lambda k: forward(0, k))
    each(4, lambda k: forward(1, k))
    all_of(all_sum.at[pl.ds(0, NX * NLEVD - 1)], rr.at[0])
    all_sum[x * NLEVD + lev] = ring_sum[...]
    scale_ref[...] = mass_scale(all_sum, target_ref)
    remap.scale = scale_ref[...]
    arrived(0)
    quarter = pltpu.make_async_copy(col_ref.at[:, :, pl.ds(32, 8)], quarter_hbm, out_sem.at[4])
    quarter.start()
    remap.unpack(from_columns(col_ref, 0))
    remap.unpack(from_columns(col_ref, 1))

    def early(j):
        remap.tile(j)
        forward(1, 4 + 2 * j)
        forward(1, 5 + 2 * j)

    each(2, early)
    each(NZ, lambda k: forward(2, k))
    arrived(1)
    remap.unpack(from_columns(col_ref, 2))
    remap.unpack(from_columns(col_ref, 4))
    remap.tile(2)
    remap.half_tile()
    outs = ((thick_ref, thick_hbm), (temp_ref, temp_hbm), (tracer_ref, tracer_hbm), (scale_ref, scale_hbm))
    stores = [pltpu.make_async_copy(a, b, out_sem.at[n]) for n, (a, b) in enumerate(outs)]
    for store in stores:
        store.start()
    all_of(ring_sum.at[pl.ds(0, NZ - 1)], ps.at[0])
    all_of(all_sum.at[pl.ds(0, NX * NLEVD - 1)], rs.at[0])
    for chunk, (first, count) in enumerate(CHUNKS):
        all_of(mid_ref.at[pl.ds(0, NX * (NZ - 1)), pl.ds(first, count)], zs.at[chunk])
        all_of(mid_ref.at[pl.ds(0, NX * NLEVD - 1), pl.ds(first, count)], fs.at[chunk])
    quarter.wait()
    for store in stores:
        store.wait()
    arrived(LAST)


def finish_kernel(
    thick_hbm, temp_hbm, tracer_hbm, late_hbm, quarter_hbm, scale_hbm, weight_hbm,
    thick_ref, temp_ref, tracer_ref,
    late_ref, quarter_ref, scale_ref, r_ref, weight_ref, sem,
):
    lat = lax.axis_index("lat")
    pairs = (
        (late_hbm, late_ref), (quarter_hbm, quarter_ref), (scale_hbm, scale_ref), (weight_hbm, weight_ref),
        (thick_hbm, thick_ref), (temp_hbm, temp_ref), (tracer_hbm, tracer_ref),
    )
    loads = [pltpu.make_async_copy(a, b, sem.at[n]) for n, (a, b) in enumerate(pairs)]
    for load in loads:
        load.start()
    for load in loads[:4]:
        load.wait()
    lane = lax.broadcasted_iota(jnp.int32, (8, 128), 1)
    remap = Remap(lat, lane, r_ref, weight_ref, thick_ref, temp_ref, tracer_ref)
    remap.scale = scale_ref[...]

    def pieces(g):
        one = [late_ref[g, x, 0:8, :] for x in range(4)]
        two = [late_ref[g, x, 8:16, :] for x in range(4)]
        return one, two, [quarter_ref[g, x] for x in range(4)], 96

    remap.unpack((0, pieces))
    for load in loads[4:]:
        load.wait()
    remap.columns(0, 8, 24 + 4 * remap.odd)


def face_below_row(first_row):
    row = lax.broadcasted_iota(jnp.int32, (8, 128), 0) * 0 + first_row
    below = jnp.sin(row.astype(F32) * np.float32(np.pi) / NLAT)
    return lanes9(below[0:1])


def row_cuts(mask_ref, cut_ref):
    row = lax.broadcasted_iota(jnp.int32, (ROWS, 128), 0)
    cuts = jnp.full((ROWS, 128), NLON, jnp.int32)
    for r in range(ROWS):
        cuts = jnp.where(row == r, jnp.where(mask_ref[r] > 0, cut_ref[r], NLON), cuts)
    return cuts


def polar_filter(flat, rows, cuts, full_ref, real_ref, uh_ref, ul_ref, z_ref):
    cos9 = [[np.float32(np.cos(2 * np.pi * a * k / 9)) for k in range(5)] for a in range(5)]
    sin9 = [[np.float32(np.sin(2 * np.pi * a * k / 9)) for k in range(5)] for a in range(5)]

    def forward(r, carry):
        at = pl.ds(pl.multiple_of(16 * r, 16), 16)
        v = [flat[at, 128 * a : 128 * a + 128] for a in range(RADIX)]
        even = [v[a] + v[9 - a] for a in range(1, 5)]
        odd = [v[a] - v[9 - a] for a in range(1, 5)]

        def put(slot, x):
            high, low = split_bf16(x)
            uh_ref[at, 128 * slot : 128 * slot + 128] = high
            ul_ref[at, 128 * slot : 128 * slot + 128] = low

        put(8, v[0] + ((even[0] + even[1]) + (even[2] + even[3])))
        for k in range(1, 5):
            put(2 * k - 2, v[0] + sum(even[a - 1] * cos9[a][k] for a in range(1, 5)))
            put(2 * k - 1, -sum(odd[a - 1] * sin9[a][k] for a in range(1, 5)))
        return carry

    lax.fori_loop(0, rows // 16, forward, 0)

    lane = lax.broadcasted_iota(jnp.int32, (rows, 128), 1)
    here = pl.ds(0, rows)
    for k in range(1, 5):
        wave = k + RADIX * lane
        keep = (jnp.minimum(wave, NLON - wave) >= cuts).astype(F32)
        keep = jnp.concatenate([keep, keep], axis=1)
        at = pl.ds(256 * (k - 1), 256)
        tables_k = full_ref[0, k - 1], full_ref[1, k - 1]
        x = dot3(uh_ref[here, at], ul_ref[here, at], *tables_k, ((1,), (0,)))
        xh, xl = split_bf16(x * keep)
        z_ref[here, at] = dot3(xh, xl, *tables_k, ((1,), (1,)))
    at = pl.ds(1024, 128)
    wave = RADIX * jnp.where(lane <= 64, lane, lane - 64)
    weight = jnp.where(jnp.logical_or(lane == 0, lane == 64), 1.0, 2.0)
    keep = jnp.where(wave >= cuts, weight, 0.0)
    x = dot3(uh_ref[here, at], ul_ref[here, at], real_ref[0], real_ref[1], ((1,), (0,)))
    xh, xl = split_bf16(x * keep)
    z_ref[here, at] = dot3(xh, xl, real_ref[0], real_ref[1], ((1,), (1,)))

    def backward(r, carry):
        at = pl.ds(pl.multiple_of(8 * r, 8), 8)
        z0 = z_ref[at, 1024:1152] * np.float32(1.0 / NLON)
        zr = [z_ref[at, 256 * k : 256 * k + 128] * np.float32(2.0 / NLON) for k in range(4)]
        zi = [z_ref[at, 256 * k + 128 : 256 * k + 256] * np.float32(2.0 / NLON) for k in range(4)]
        flat[at, 0:128] = flat[at, 0:128] - (z0 + ((zr[0] + zr[1]) + (zr[2] + zr[3])))
        for a in range(1, 5):
            even = z0 + sum(zr[k - 1] * cos9[a][k] for k in range(1, 5))
            odd = sum(zi[k - 1] * sin9[a][k] for k in range(1, 5))
            lo, hi = pl.ds(128 * a, 128), pl.ds(128 * (9 - a), 128)
            flat[at, lo] = flat[at, lo] - (even - odd)
            flat[at, hi] = flat[at, hi] - (even + odd)
        return carry

    lax.fori_loop(0, rows // 8, backward, 0)


ACROSS = (0, 1, 3, 2)
CHUNKS = ((0, 40), (56, 28), (40, 16))
TILE_ROW = (0, 8, 56, 40)
TILE_STEP = (16, 16, 8, 8)


LAST = 2


def mass_scale(all_sum, target_ref):
    area = float(np.sum(np.sin((np.arange(NLAT) + 0.5) * np.pi / NLAT)))
    total = jnp.sum(all_sum[...].reshape(NX * NLEVD * NZ, 128), axis=0, keepdims=True)
    total = jnp.sum(total, axis=1, keepdims=True)
    return jnp.broadcast_to(target_ref[0] * (NLON * area) / total, (8, 128))


def from_columns(col_ref, j):
    def pieces(g):
        if j < 4:
            one = [col_ref[g, x, pl.ds(TILE_ROW[j], 8), :] for x in range(4)]
            two = [col_ref[g, x, pl.ds(TILE_ROW[j] + TILE_STEP[j], 8), :] for x in range(4)]
            return one, two, [col_ref[g, x, 32:40, :] for x in range(4)], 32 * j
        one = [col_ref[g, x, 72:80, :] for x in range(4)]
        two = [pltpu.roll(v, 4, 0) for v in one]
        last = [col_ref[g, x, 80:84, :] for x in range(4)]
        return one, two, [jnp.concatenate([v, v], axis=0) for v in last], 0

    return j, pieces


class Remap:
    def __init__(self, lat, lane, r_ref, weight_ref, thick_ref, temp_ref, tracer_ref):
        self.odd = lax.rem(lat, 2)
        self.lane = lane
        self.r_ref = r_ref
        self.outs = thick_ref, temp_ref, tracer_ref
        self.weights = [weight_ref[k] for k in range(LEV)]
        whole = self.weights[0]
        for k in range(1, LEV):
            whole = whole + self.weights[k]
        self.whole = whole

    def unpack(self, tile):
        lane, r_ref = self.lane, self.r_ref
        j, pieces = tile

        def merge(parts):
            return jnp.where(
                lane < 48, jnp.where(lane < 24, parts[0], parts[1]), jnp.where(lane < 72, parts[2], parts[3])
            )

        def move(v, source, target):
            amount = (target - source) % 128
            return v if amount == 0 else pltpu.roll(v, amount, 1)

        phase = jnp.where(
            lane >= 72, lane - 72, jnp.where(lane >= 48, lane - 48, jnp.where(lane >= 24, lane - 24, lane))
        )

        def body(g, carry):
            one, two, last, lane0 = pieces(g)

            def put(fl, v):
                r_ref[fl // 4, g * 4 + fl % 4, 8 * j : 8 * j + 8, :] = v

            for n in range(5):
                put(n, merge([move(one[x], 24 * n, 24 * x) for x in range(4)]))
                put(5 + n, merge([move(two[x], 24 * n, 24 * x) for x in range(4)]))
            put(10, merge([move(last[x], lane0, 24 * x) for x in range(4)]))
            a = merge([move(one[x], 120, 24 * x) for x in range(4)])
            b = merge([move(two[x], 120, 24 * x + 8) for x in range(4)])
            c = merge([move(last[x], lane0 + 24, 24 * x + 16) for x in range(4)])
            put(11, jnp.where(phase < 8, a, jnp.where(phase < 16, b, c)))
            return carry

        lax.fori_loop(0, NLEVD, body, 0)

    def tile(self, j):
        self.columns(j, 8, 8 * j + 4 * self.odd)

    def half_tile(self):
        self.columns(4, 4, 32 - 32 * self.odd)

    def columns(self, j, count, lon0):
        weights, r_ref = self.weights, self.r_ref
        thick_ref, temp_ref, tracer_ref = self.outs
        at = pl.ds(pl.multiple_of(8 * j, 8), 8)
        surface = r_ref[0, 0, at, :]
        for m in range(1, LEV):
            surface = surface + r_ref[0, m, at, :]
        unit = surface / jnp.full((8, 128), self.whole)
        previous = (jnp.zeros((8, 128), F32), jnp.zeros((8, 128), F32))
        running = None
        for k0 in range(0, LEV, 8):
            bounds = []
            for k in range(k0, k0 + 8):
                running = weights[k] if running is None else running + weights[k]
                bounds.append(unit * running)
            temps = [jnp.zeros((8, 128), F32)] * 8
            tracs = [jnp.zeros((8, 128), F32)] * 8
            top = jnp.zeros((8, 128), F32)
            for m in range(LEV):
                th = r_ref[0, m, at, :]
                te = r_ref[1, m, at, :]
                tr = r_ref[2, m, at, :]
                for n in range(8):
                    part = jnp.minimum(jnp.maximum(bounds[n] - top, 0.0), th)
                    temps[n] = temps[n] + te * part
                    tracs[n] = tracs[n] + tr * part
                top = top + th
            for n in range(8):
                k = k0 + n
                target = unit * weights[k]
                inverse = 1.0 / target
                rows = pl.ds(lon0 * LEV + k, count, stride=LEV)
                thick_ref[rows, :] = (target * self.scale)[0:count, 0:96]
                temp_ref[rows, :] = ((temps[n] - previous[0]) * inverse)[0:count, 0:96]
                tracer_ref[rows, :] = ((tracs[n] - previous[1]) * inverse)[0:count, 0:96]
                previous = (temps[n], tracs[n])


def on_device(th, te, tr, ec, nc, polar_mask, wave_cutoff, level_weight, target_surface):
    vmem = pl.BlockSpec(memory_space=pltpu.VMEM)
    hbm = pl.BlockSpec(memory_space=pl.ANY)
    full, real = tables()
    dma = pltpu.SemaphoreType.DMA
    chunks = len(CHUNKS)
    fields = tuple(jax.ShapeDtypeStruct((36 * LEV, 96), F32) for _ in range(3))
    late = jax.ShapeDtypeStruct((NLEVD, NX, 16, 128), F32)
    quarter = jax.ShapeDtypeStruct((NLEVD, NX, 8, 128), F32)
    scale = jax.ShapeDtypeStruct((8, 128), F32)
    parts = pl.pallas_call(
        step_kernel,
        name="step",
        out_shape=fields + (late, quarter, scale),
        in_specs=[hbm] * 11,
        out_specs=(hbm,) * 6,
        scratch_shapes=[pltpu.VMEM(o.shape, F32) for o in fields + (scale,)]
        + [
            pltpu.VMEM((5, LEVD, ROWS, NLON), F32),
            pltpu.VMEM(full.shape, BF16),
            pltpu.VMEM(real.shape, BF16),
            pltpu.VMEM((3, LEVD, ROWS, NLON), F32),
            pltpu.VMEM((16, NLON), F32),
            pltpu.VMEM((12, NLON), F32),
            pltpu.VMEM((16, NLON), F32),
            pltpu.VMEM((12, NLON), F32),
            pltpu.VMEM((32, NLON), F32),
            pltpu.VMEM((288, NLON), BF16),
            pltpu.VMEM((288, NLON), BF16),
            pltpu.VMEM((288, NLON), F32),
            pltpu.VMEM((3, NLON, 128), F32),
            pltpu.VMEM((NLATD, SENT, 128), F32),
            pltpu.VMEM((NLATD, SENT, 128), F32),
            pltpu.VMEM((NLEVD, NX, SENT, 128), F32),
            pltpu.VMEM((1, 128), F32),
            pltpu.VMEM((NZ, 1, 128), F32),
            pltpu.VMEM((NX * NLEVD, NZ, 1, 128), F32),
            pltpu.VMEM((3, LEV, 40, 128), F32),
            dma((11,)), dma((2,)), dma((2,)), dma((1,)),
            dma((chunks,)), dma((chunks, NZ)), dma((1,)), dma((1,)), dma((1,)), dma((1,)),
            dma((chunks,)), dma((chunks,)),
            pltpu.SMEM((ROWS,), jnp.int32), pltpu.SMEM((ROWS,), jnp.int32),
            pltpu.SMEM((LEV,), F32), pltpu.SMEM((1,), F32), dma((5,)),
        ],
        compiler_params=pltpu.CompilerParams(
            collective_id=0, has_side_effects=True, vmem_limit_bytes=67043328
        ),
    )(th, te, tr, ec, nc, polar_mask, wave_cutoff, level_weight, target_surface, jnp.asarray(full), jnp.asarray(real))
    outs = pl.pallas_call(
        finish_kernel,
        name="finish",
        out_shape=fields,
        in_specs=[hbm] * 7,
        out_specs=(vmem,) * 3,
        scratch_shapes=[
            pltpu.VMEM(late.shape, F32), pltpu.VMEM(quarter.shape, F32), pltpu.VMEM(scale.shape, F32),
            pltpu.VMEM((3, LEV, 8, 128), F32), pltpu.SMEM((LEV,), F32), dma((7,)),
        ],
        compiler_params=pltpu.CompilerParams(vmem_limit_bytes=67043328),
    )(*parts, level_weight)
    return tuple(o.reshape(36, LEV, 96).transpose(1, 2, 0) for o in outs)


def solution(mesh):
    field = P("lev", "lat", None)
    return jax.shard_map(
        on_device,
        mesh=mesh,
        in_specs=(field,) * 5 + (P("lat"), P("lat"), P(), P()),
        out_specs=(P(None, "lev", "lat"),) * 3,
        check_vma=False,
    )
```

```python
import functools

import jax
import jax.numpy as jnp
import numpy as np
from jax import lax
from jax.experimental import pallas as pl
from jax.experimental.pallas import tpu as pltpu
from jax.sharding import PartitionSpec as P

MESH = pl.DeviceIdType.MESH
F32 = jnp.float32
BF16 = jnp.bfloat16

NLON, NLAT, LEV = 1152, 768, 32
ROWS = 24
LEVD = 4
NZ, NX, NY = 8, 4, 4
NLATD, NLEVD = 32, 8
RADIX, POINTS = 9, 128
SENT = 84
POLAR_BANDS = -(-(NLAT // 5) // ROWS)


def split_bf16(x):
    high = x.astype(BF16)
    return high, (x - high.astype(F32)).astype(BF16)


def tables():
    b = np.arange(POINTS)[:, None]
    full = np.zeros((4, 256, 256))
    for k1 in range(1, 5):
        angle = 2.0 * np.pi * ((b * (k1 + RADIX * np.arange(POINTS)[None, :])) % NLON) / NLON
        c, s = np.cos(angle), np.sin(angle)
        full[k1 - 1] = np.block([[c, -s], [s, c]])
    col = np.arange(POINTS)[None, :]
    wave = np.where(col <= 64, col, col - 64)
    angle = 2.0 * np.pi * ((b * wave) % POINTS) / POINTS
    real = np.where(col <= 64, np.cos(angle), np.sin(angle))

    def pair(x):
        high = x.astype(np.float32).astype(BF16)
        low = (x - high.astype(np.float64)).astype(np.float32).astype(BF16)
        return np.stack([np.asarray(high), np.asarray(low)])

    return pair(full), pair(real)


def dot3(xh, xl, th, tl, dims):
    dot = functools.partial(
        lax.dot_general, dimension_numbers=(dims, ((), ())), preferred_element_type=F32
    )
    rows = xh.shape[0]
    both = dot(jnp.concatenate([xh, xl], axis=0), th)
    return both[:rows] + both[rows:] + dot(xh, tl)


def lanes9(x):
    return jnp.concatenate([x] * RADIX, axis=1)


def step_kernel(
    th_hbm, te_hbm, tr_hbm, ec_hbm, nc_hbm, mask_hbm, cut_hbm, weight_hbm, target_hbm, full_hbm, real_hbm,
    thick_hbm, temp_hbm, tracer_hbm, late_hbm, quarter_hbm, scale_hbm,
    thick_ref, temp_ref, tracer_ref, scale_ref,
    in_ref, full_ref, real_ref, s_ref, up_ref, down_ref, from_south, from_north, edge_ref, uh_ref, ul_ref, z_ref, t_ref,
    msg_ref, mid_ref, col_ref, part_ref, ring_sum, all_sum, r_ref,
    load_sem, halo_send, halo_recv, own_sem, zs, zr, ps, pr, rs, rr, fs, fr,
    mask_ref, cut_ref, weight_ref, target_ref, out_sem,
):
    lat = lax.axis_index("lat")
    lev = lax.axis_index("lev")
    z, x = lat // NX, lax.rem(lat, NX)
    north = lax.rem(lat + 1, NLATD)
    south = lax.rem(lat + NLATD - 1, NLATD)
    polar = jnp.logical_or(lat < POLAR_BANDS, lat >= NLATD - POLAR_BANDS)

    fields_hbm = (th_hbm, te_hbm, tr_hbm, nc_hbm, ec_hbm)
    loads = [pltpu.make_async_copy(fields_hbm[f], in_ref.at[f], load_sem.at[f]) for f in range(5)]
    small = ((mask_hbm, mask_ref), (cut_hbm, cut_ref), (weight_hbm, weight_ref), (target_hbm, target_ref))
    loads += [pltpu.make_async_copy(a, b, load_sem.at[7 + n]) for n, (a, b) in enumerate(small)]
    for load in loads:
        load.start()
    barrier = pltpu.get_barrier_semaphore()
    for other in (north, south):
        pl.semaphore_signal(barrier, inc=1, device_id=(other, lev), device_id_type=MESH)

    def plane_peer(o):
        return z * NX + lax.rem(x + o // NLEVD, NX), lax.rem(lev + o, NLEVD)

    def greet_plane(o, carry):
        pl.semaphore_signal(barrier, inc=1, device_id=plane_peer(o), device_id_type=MESH)
        return carry

    def greet_ring(o, carry):
        peer = (lax.rem(lat + NX * o, NLATD), lev)
        pl.semaphore_signal(barrier, inc=1, device_id=peer, device_id_type=MESH)
        return carry

    lax.fori_loop(1, NZ, greet_ring, 0)
    lax.fori_loop(1, NX * NLEVD, greet_plane, 0)

    table_loads = (
        pltpu.make_async_copy(full_hbm, full_ref, load_sem.at[5]),
        pltpu.make_async_copy(real_hbm, real_ref, load_sem.at[6]),
    )

    @pl.when(polar)
    def _():
        for load in table_loads:
            load.start()

    for load in loads:
        load.wait()
    th_ref, te_ref, tr_ref, nc_ref, ec_ref = (in_ref.at[f] for f in range(5))
    fields = (th_ref, te_ref, tr_ref, nc_ref)
    for f in range(4):
        for l in range(LEVD):
            up_ref[pl.ds(4 * f + l, 1), :] = fields[f][l, ROWS - 1 : ROWS, :]
            if f < 3:
                down_ref[pl.ds(4 * f + l, 1), :] = fields[f][l, 0:1, :]

    def east(l, carry):
        th, te, tr = th_ref[l], te_ref[l], tr_ref[l]
        mass = ec_ref[l] * (th + pltpu.roll(th, NLON - 1, 1)) * 0.5
        temp = mass * (te + pltpu.roll(te, NLON - 1, 1)) * 0.5
        trac = mass * (tr + pltpu.roll(tr, NLON - 1, 1)) * 0.5
        s_ref[0, l] = pltpu.roll(mass, 1, 1) - mass
        s_ref[1, l] = pltpu.roll(temp, 1, 1) - temp
        s_ref[2, l] = pltpu.roll(trac, 1, 1) - trac
        return carry

    lax.fori_loop(0, LEVD, east, 0)

    first_row = lat * ROWS
    row = (first_row + lax.broadcasted_iota(jnp.int32, (ROWS, 128), 0)).astype(F32)
    center = lanes9(jnp.sin((row + 0.5) * np.float32(np.pi) / NLAT))
    face = lanes9(jnp.sin((row + 1.0) * np.float32(np.pi) / NLAT))
    inverse_center = 1.0 / center
    row_in = lax.broadcasted_iota(jnp.int32, (ROWS, NLON), 0)

    def inner(l, carry):
        th, te, tr = th_ref[l], te_ref[l], tr_ref[l]

        def above(v):
            return pltpu.roll(v, ROWS - 1, 0)

        mass = nc_ref[l] * (th + above(th)) * 0.5 * face
        mass = jnp.where(row_in == ROWS - 1, 0.0, mass)
        temp = mass * (te + above(te)) * 0.5
        trac = mass * (tr + above(tr)) * 0.5
        for f, flux in enumerate((mass, temp, trac)):
            s_ref[f, l] = s_ref[f, l] - (flux - pltpu.roll(flux, 1, 0)) * inverse_center
        return carry

    lax.fori_loop(0, LEVD, inner, 0)
    flat = s_ref.reshape(3 * LEVD * ROWS, NLON)
    scratch = full_ref, real_ref, uh_ref, ul_ref, z_ref

    @pl.when(polar)
    def _():
        for load in table_loads:
            load.wait()
        cuts = row_cuts(mask_ref, cut_ref)
        polar_filter(flat, 3 * LEVD * ROWS, jnp.concatenate([cuts] * (3 * LEVD), axis=0), *scratch)

    pl.semaphore_wait(barrier, 2 + NZ - 1 + NX * NLEVD - 1)
    to_north = pltpu.make_async_remote_copy(
        src_ref=up_ref, dst_ref=from_south, send_sem=halo_send.at[0], recv_sem=halo_recv.at[0],
        device_id=(north, lev), device_id_type=MESH,
    )
    to_south = pltpu.make_async_remote_copy(
        src_ref=down_ref, dst_ref=from_north, send_sem=halo_send.at[1], recv_sem=halo_recv.at[1],
        device_id=(south, lev), device_id_type=MESH,
    )
    has_north, has_south = lat < NLATD - 1, lat > 0
    pl.when(has_north)(to_north.start)
    pl.when(has_south)(to_south.start)
    pl.when(has_south)(to_north.wait_recv)
    pl.when(has_north)(to_south.wait_recv)

    def rows_of(ref, f):
        return ref[4 * f : 4 * f + 4, :]

    def beyond(ref, f, there):
        return jnp.where(there, rows_of(ref, f), 0.0)

    def faces(courant, own, other, face_row):
        mass = courant * (own[0] + other[0]) * 0.5 * face_row
        return mass, mass * (own[1] + other[1]) * 0.5, mass * (own[2] + other[2]) * 0.5

    top = faces(
        rows_of(up_ref, 3), [rows_of(up_ref, f) for f in range(3)],
        [beyond(from_north, f, has_north) for f in range(3)], face[ROWS - 1 : ROWS],
    )
    bottom = faces(
        beyond(from_south, 3, has_south), [beyond(from_south, f, has_south) for f in range(3)],
        [rows_of(down_ref, f) for f in range(3)], face_below_row(first_row),
    )
    for f in range(3):
        edge_ref[4 * f : 4 * f + 4, :] = -top[f] * inverse_center[ROWS - 1 : ROWS]
        edge_ref[12 + 4 * f : 16 + 4 * f, :] = bottom[f] * inverse_center[0:1]
    edge_ref[24:32, :] = jnp.zeros((8, NLON), F32)

    @pl.when(polar)
    def _():
        cuts = row_cuts(mask_ref, cut_ref)
        edge_row = lax.broadcasted_iota(jnp.int32, (32, 128), 0)
        cuts = jnp.where(edge_row < 12, cuts[ROWS - 1 : ROWS], cuts[0:1])
        polar_filter(edge_ref, 32, cuts, *scratch)

    for f in range(3):
        for l in range(LEVD):
            n = 4 * f + l
            s_ref[f, l, ROWS - 1 : ROWS, :] = s_ref[f, l, ROWS - 1 : ROWS, :] + edge_ref[n : n + 1, :]
            s_ref[f, l, 0:1, :] = s_ref[f, l, 0:1, :] + edge_ref[12 + n : 13 + n, :]
    pl.when(has_north)(to_north.wait_send)
    pl.when(has_south)(to_south.wait_send)

    def update(l, total):
        th, te, tr = th_ref[l], te_ref[l], tr_ref[l]
        mass = s_ref[0, l]
        inverse = 1.0 / th
        new_th = th + mass
        s_ref[0, l] = new_th
        s_ref[1, l] = te + (s_ref[1, l] - te * mass) * inverse
        s_ref[2, l] = tr + (s_ref[2, l] - tr * mass) * inverse
        weighted = new_th * center
        for a in range(RADIX):
            part = weighted[:, 128 * a : 128 * a + 128]
            total = total + (part[0:8] + part[8:16] + part[16:24])
        return total

    total = lax.fori_loop(0, LEVD, update, jnp.zeros((8, 128), F32))
    total = jnp.sum(total, axis=0, keepdims=True)
    part_ref[...] = total
    ring_sum[z] = total

    for a in range(RADIX):
        at = pl.ds(128 * a, 128)
        one = jnp.concatenate([flat[0:120, at], flat[264:272, at]], axis=0)
        two = jnp.concatenate([flat[120:240, at], flat[272:280, at]], axis=0)
        last = jnp.concatenate([flat[240:264, at], flat[280:288, at]], axis=0)
        t_ref[0, at, :] = one.T
        t_ref[1, at, :] = two.T
        t_ref[2, at, :] = jnp.concatenate([last] * 4, axis=0).T

    sub = lax.broadcasted_iota(jnp.int32, (8, 128), 0)
    lane = lax.broadcasted_iota(jnp.int32, (8, 128), 1)

    def pack(p, carry):
        base = 72 * p

        def tile(q, j, n=1):
            return t_ref[q, pl.ds(pl.multiple_of(base + 8 * j, 8), 8 * n), :]

        def fours(u):
            return jnp.where(
                lane < 64, jnp.where(lane < 32, u[0], u[1]), jnp.where(lane < 96, u[2], u[3])
            )

        for q in range(2):
            for j in range(4):
                at = pl.ds(TILE_ROW[j] + TILE_STEP[j] * q, 8)
                msg_ref[2 * p, at, :] = tile(q, j)
                msg_ref[2 * p + 1, at, :] = tile(q, 5 + j)
        t0, t1, t2 = tile(0, 4), tile(1, 4), tile(2, 4)
        msg_ref[2 * p, 72:80, :] = jnp.where(sub < 4, t0, pltpu.roll(t1, 4, 0))
        msg_ref[2 * p + 1, 72:80, :] = jnp.where(sub < 4, pltpu.roll(t0, 4, 0), t1)
        msg_ref[2 * p, 32:40, :] = fours([tile(2, j) for j in range(4)])
        msg_ref[2 * p + 1, 32:40, :] = fours([tile(2, j) for j in range(5, 9)])
        msg_ref[2 * p, 80:84, :] = t2[0:4]
        msg_ref[2 * p + 1, 80:84, :] = pltpu.roll(t2, 4, 0)[0:4]
        return carry

    lax.fori_loop(0, NLATD // 2, pack, 0)

    def ring_part(o):
        return pltpu.make_async_remote_copy(
            src_ref=part_ref, dst_ref=ring_sum.at[z], send_sem=ps.at[0], recv_sem=pr.at[0],
            device_id=(lax.rem(lat + NX * o, NLATD), lev), device_id_type=MESH,
        )

    def plane_part(o):
        return pltpu.make_async_remote_copy(
            src_ref=ring_sum, dst_ref=all_sum.at[x * NLEVD + lev], send_sem=rs.at[0], recv_sem=rr.at[0],
            device_id=plane_peer(o), device_id_type=MESH,
        )

    def all_of(ref, sem):
        pltpu.make_async_copy(ref, ref, sem).wait()

    def each(count, action, start=0):
        def body(o, carry):
            action(o)
            return carry

        lax.fori_loop(start, count, body, 0)

    each(NZ, lambda o: ring_part(o).start(), 1)

    def distance(k):
        return jnp.where(lax.rem(k, 2) == 1, (k + 1) // 2, lax.rem(NZ - k // 2, NZ))

    def along_z(chunk, k):
        to = lax.rem(z + distance(k), NZ)
        first, count = CHUNKS[chunk]
        return pltpu.make_async_remote_copy(
            src_ref=msg_ref.at[pl.ds(NX * to, NX), pl.ds(first, count)],
            dst_ref=mid_ref.at[pl.ds(NX * z, NX), pl.ds(first, count)],
            send_sem=zs.at[chunk], recv_sem=zr.at[chunk, k],
            device_id=(to * NX + x, lev), device_id_type=MESH,
        )

    for chunk in range(len(CHUNKS)):
        each(NZ, lambda k: along_z(chunk, k).start(), 1)
    mine = pltpu.make_async_copy(
        msg_ref.at[pl.ds(NX * z, NX)], mid_ref.at[pl.ds(NX * z, NX)], own_sem.at[0]
    )
    mine.start()

    mine.wait()

    def onward(chunk, source, to_x):
        first, count = CHUNKS[chunk]
        piece = mid_ref.at[NX * source + to_x, pl.ds(first, count)]
        place = late_hbm.at[lev, x] if chunk == LAST else col_ref.at[lev, x, pl.ds(first, count)]
        away = pltpu.make_async_remote_copy(
            src_ref=piece, dst_ref=place, send_sem=fs.at[chunk], recv_sem=fr.at[chunk],
            device_id=(z * NX + to_x, source), device_id_type=MESH,
        )
        stay = pltpu.make_async_copy(piece, place, fr.at[chunk])
        return away, stay

    def forward(chunk, k):
        source = lax.rem(z + NZ - distance(k), NZ)

        @pl.when(k > 0)
        def _():
            along_z(chunk, k).wait_recv()

        for dx in ACROSS:
            away, stay = onward(chunk, source, lax.rem(x + dx, NX))
            if dx == 0:
                pl.when(source != lev)(away.start)
                pl.when(source == lev)(stay.start)
            else:
                away.start()

    def arrived(chunk):
        first, count = CHUNKS[chunk]
        all_of(mid_ref.at[:, pl.ds(first, count)], fr.at[chunk])

    remap = Remap(lat, lane, r_ref, weight_ref, thick_ref, temp_ref, tracer_ref)

    each(1, lambda k: forward(0, k))
    all_of(ring_sum.at[pl.ds(0, NZ - 1)], pr.at[0])
    each(NX * NLEVD, lambda o: plane_part(o).start(), 1)
    each(NZ, lambda k: forward(0, k), 1)
    each(NZ, lambda k: forward(1, k))
    all_of(all_sum.at[pl.ds(0, NX * NLEVD - 1)], rr.at[0])
    all_sum[x * NLEVD + lev] = ring_sum[...]
    scale_ref[...] = mass_scale(all_sum, target_ref)
    remap.scale = scale_ref[...]
    arrived(0)
    quarter = pltpu.make_async_copy(col_ref.at[:, :, pl.ds(32, 8)], quarter_hbm, out_sem.at[4])
    quarter.start()
    remap.unpack(from_columns(col_ref, 0))
    remap.tile(0)
    remap.unpack(from_columns(col_ref, 1))
    remap.tile(1)
    each(NZ, lambda k: forward(2, k))
    arrived(1)
    remap.unpack(from_columns(col_ref, 2))
    remap.tile(2)
    remap.unpack(from_columns(col_ref, 4))
    remap.half_tile()
    outs = ((thick_ref, thick_hbm), (temp_ref, temp_hbm), (tracer_ref, tracer_hbm), (scale_ref, scale_hbm))
    stores = [pltpu.make_async_copy(a, b, out_sem.at[n]) for n, (a, b) in enumerate(outs)]
    for store in stores:
        store.start()
    all_of(ring_sum.at[pl.ds(0, NZ - 1)], ps.at[0])
    all_of(all_sum.at[pl.ds(0, NX * NLEVD - 1)], rs.at[0])
    for chunk, (first, count) in enumerate(CHUNKS):
        all_of(mid_ref.at[pl.ds(0, NX * (NZ - 1)), pl.ds(first, count)], zs.at[chunk])
        all_of(mid_ref.at[pl.ds(0, NX * NLEVD - 1), pl.ds(first, count)], fs.at[chunk])
    quarter.wait()
    for store in stores:
        store.wait()
    arrived(LAST)


def finish_kernel(
    thick_hbm, temp_hbm, tracer_hbm, late_hbm, quarter_hbm, scale_hbm, weight_hbm,
    thick_ref, temp_ref, tracer_ref,
    late_ref, quarter_ref, scale_ref, r_ref, weight_ref, sem,
):
    lat = lax.axis_index("lat")
    pairs = (
        (late_hbm, late_ref), (quarter_hbm, quarter_ref), (scale_hbm, scale_ref), (weight_hbm, weight_ref),
        (thick_hbm, thick_ref), (temp_hbm, temp_ref), (tracer_hbm, tracer_ref),
    )
    loads = [pltpu.make_async_copy(a, b, sem.at[n]) for n, (a, b) in enumerate(pairs)]
    for load in loads:
        load.start()
    for load in loads[:4]:
        load.wait()
    lane = lax.broadcasted_iota(jnp.int32, (8, 128), 1)
    remap = Remap(lat, lane, r_ref, weight_ref, thick_ref, temp_ref, tracer_ref)
    remap.scale = scale_ref[...]

    def pieces(g):
        one = [late_ref[g, x, 0:8, :] for x in range(4)]
        two = [late_ref[g, x, 8:16, :] for x in range(4)]
        return one, two, [quarter_ref[g, x] for x in range(4)], 96

    remap.unpack((0, pieces))
    for load in loads[4:]:
        load.wait()
    remap.columns(0, 8, 24 + 4 * remap.odd)


def face_below_row(first_row):
    row = lax.broadcasted_iota(jnp.int32, (8, 128), 0) * 0 + first_row
    below = jnp.sin(row.astype(F32) * np.float32(np.pi) / NLAT)
    return lanes9(below[0:1])


def row_cuts(mask_ref, cut_ref):
    row = lax.broadcasted_iota(jnp.int32, (ROWS, 128), 0)
    cuts = jnp.full((ROWS, 128), NLON, jnp.int32)
    for r in range(ROWS):
        cuts = jnp.where(row == r, jnp.where(mask_ref[r] > 0, cut_ref[r], NLON), cuts)
    return cuts


def polar_filter(flat, rows, cuts, full_ref, real_ref, uh_ref, ul_ref, z_ref):
    cos9 = [[np.float32(np.cos(2 * np.pi * a * k / 9)) for k in range(5)] for a in range(5)]
    sin9 = [[np.float32(np.sin(2 * np.pi * a * k / 9)) for k in range(5)] for a in range(5)]

    def forward(r, carry):
        at = pl.ds(pl.multiple_of(16 * r, 16), 16)
        v = [flat[at, 128 * a : 128 * a + 128] for a in range(RADIX)]
        even = [v[a] + v[9 - a] for a in range(1, 5)]
        odd = [v[a] - v[9 - a] for a in range(1, 5)]

        def put(slot, x):
            high, low = split_bf16(x)
            uh_ref[at, 128 * slot : 128 * slot + 128] = high
            ul_ref[at, 128 * slot : 128 * slot + 128] = low

        put(8, v[0] + ((even[0] + even[1]) + (even[2] + even[3])))
        for k in range(1, 5):
            put(2 * k - 2, v[0] + sum(even[a - 1] * cos9[a][k] for a in range(1, 5)))
            put(2 * k - 1, -sum(odd[a - 1] * sin9[a][k] for a in range(1, 5)))
        return carry

    lax.fori_loop(0, rows // 16, forward, 0)

    lane = lax.broadcasted_iota(jnp.int32, (rows, 128), 1)
    here = pl.ds(0, rows)
    for k in range(1, 5):
        wave = k + RADIX * lane
        keep = (jnp.minimum(wave, NLON - wave) >= cuts).astype(F32)
        keep = jnp.concatenate([keep, keep], axis=1)
        at = pl.ds(256 * (k - 1), 256)
        tables_k = full_ref[0, k - 1], full_ref[1, k - 1]
        x = dot3(uh_ref[here, at], ul_ref[here, at], *tables_k, ((1,), (0,)))
        xh, xl = split_bf16(x * keep)
        z_ref[here, at] = dot3(xh, xl, *tables_k, ((1,), (1,)))
    at = pl.ds(1024, 128)
    wave = RADIX * jnp.where(lane <= 64, lane, lane - 64)
    weight = jnp.where(jnp.logical_or(lane == 0, lane == 64), 1.0, 2.0)
    keep = jnp.where(wave >= cuts, weight, 0.0)
    x = dot3(uh_ref[here, at], ul_ref[here, at], real_ref[0], real_ref[1], ((1,), (0,)))
    xh, xl = split_bf16(x * keep)
    z_ref[here, at] = dot3(xh, xl, real_ref[0], real_ref[1], ((1,), (1,)))

    def backward(r, carry):
        at = pl.ds(pl.multiple_of(8 * r, 8), 8)
        z0 = z_ref[at, 1024:1152] * np.float32(1.0 / NLON)
        zr = [z_ref[at, 256 * k : 256 * k + 128] * np.float32(2.0 / NLON) for k in range(4)]
        zi = [z_ref[at, 256 * k + 128 : 256 * k + 256] * np.float32(2.0 / NLON) for k in range(4)]
        flat[at, 0:128] = flat[at, 0:128] - (z0 + ((zr[0] + zr[1]) + (zr[2] + zr[3])))
        for a in range(1, 5):
            even = z0 + sum(zr[k - 1] * cos9[a][k] for k in range(1, 5))
            odd = sum(zi[k - 1] * sin9[a][k] for k in range(1, 5))
            lo, hi = pl.ds(128 * a, 128), pl.ds(128 * (9 - a), 128)
            flat[at, lo] = flat[at, lo] - (even - odd)
            flat[at, hi] = flat[at, hi] - (even + odd)
        return carry

    lax.fori_loop(0, rows // 8, backward, 0)


ACROSS = (0, 1, 3, 2)
CHUNKS = ((0, 40), (56, 28), (40, 16))
TILE_ROW = (0, 8, 56, 40)
TILE_STEP = (16, 16, 8, 8)


LAST = 2


def mass_scale(all_sum, target_ref):
    area = float(np.sum(np.sin((np.arange(NLAT) + 0.5) * np.pi / NLAT)))
    total = jnp.sum(all_sum[...].reshape(NX * NLEVD * NZ, 128), axis=0, keepdims=True)
    total = jnp.sum(total, axis=1, keepdims=True)
    return jnp.broadcast_to(target_ref[0] * (NLON * area) / total, (8, 128))


def from_columns(col_ref, j):
    def pieces(g):
        if j < 4:
            one = [col_ref[g, x, pl.ds(TILE_ROW[j], 8), :] for x in range(4)]
            two = [col_ref[g, x, pl.ds(TILE_ROW[j] + TILE_STEP[j], 8), :] for x in range(4)]
            return one, two, [col_ref[g, x, 32:40, :] for x in range(4)], 32 * j
        one = [col_ref[g, x, 72:80, :] for x in range(4)]
        two = [pltpu.roll(v, 4, 0) for v in one]
        last = [col_ref[g, x, 80:84, :] for x in range(4)]
        return one, two, [jnp.concatenate([v, v], axis=0) for v in last], 0

    return j, pieces


class Remap:
    def __init__(self, lat, lane, r_ref, weight_ref, thick_ref, temp_ref, tracer_ref):
        self.odd = lax.rem(lat, 2)
        self.lane = lane
        self.r_ref = r_ref
        self.outs = thick_ref, temp_ref, tracer_ref
        self.weights = [weight_ref[k] for k in range(LEV)]
        whole = self.weights[0]
        for k in range(1, LEV):
            whole = whole + self.weights[k]
        self.whole = whole

    def unpack(self, tile):
        lane, r_ref = self.lane, self.r_ref
        j, pieces = tile

        def merge(parts):
            return jnp.where(
                lane < 48, jnp.where(lane < 24, parts[0], parts[1]), jnp.where(lane < 72, parts[2], parts[3])
            )

        def move(v, source, target):
            amount = (target - source) % 128
            return v if amount == 0 else pltpu.roll(v, amount, 1)

        phase = jnp.where(
            lane >= 72, lane - 72, jnp.where(lane >= 48, lane - 48, jnp.where(lane >= 24, lane - 24, lane))
        )

        def body(g, carry):
            one, two, last, lane0 = pieces(g)

            def put(fl, v):
                r_ref[fl // 4, g * 4 + fl % 4, 8 * j : 8 * j + 8, :] = v

            for n in range(5):
                put(n, merge([move(one[x], 24 * n, 24 * x) for x in range(4)]))
                put(5 + n, merge([move(two[x], 24 * n, 24 * x) for x in range(4)]))
            put(10, merge([move(last[x], lane0, 24 * x) for x in range(4)]))
            a = merge([move(one[x], 120, 24 * x) for x in range(4)])
            b = merge([move(two[x], 120, 24 * x + 8) for x in range(4)])
            c = merge([move(last[x], lane0 + 24, 24 * x + 16) for x in range(4)])
            put(11, jnp.where(phase < 8, a, jnp.where(phase < 16, b, c)))
            return carry

        lax.fori_loop(0, NLEVD, body, 0)

    def tile(self, j):
        self.columns(j, 8, 8 * j + 4 * self.odd)

    def half_tile(self):
        self.columns(4, 4, 32 - 32 * self.odd)

    def columns(self, j, count, lon0):
        weights, r_ref = self.weights, self.r_ref
        thick_ref, temp_ref, tracer_ref = self.outs
        at = pl.ds(pl.multiple_of(8 * j, 8), 8)
        surface = r_ref[0, 0, at, :]
        for m in range(1, LEV):
            surface = surface + r_ref[0, m, at, :]
        unit = surface / jnp.full((8, 128), self.whole)
        previous = (jnp.zeros((8, 128), F32), jnp.zeros((8, 128), F32))
        running = None
        for k0 in range(0, LEV, 8):
            bounds = []
            for k in range(k0, k0 + 8):
                running = weights[k] if running is None else running + weights[k]
                bounds.append(unit * running)
            temps = [jnp.zeros((8, 128), F32)] * 8
            tracs = [jnp.zeros((8, 128), F32)] * 8
            top = jnp.zeros((8, 128), F32)
            for m in range(LEV):
                th = r_ref[0, m, at, :]
                te = r_ref[1, m, at, :]
                tr = r_ref[2, m, at, :]
                for n in range(8):
                    part = jnp.minimum(jnp.maximum(bounds[n] - top, 0.0), th)
                    temps[n] = temps[n] + te * part
                    tracs[n] = tracs[n] + tr * part
                top = top + th
            for n in range(8):
                k = k0 + n
                target = unit * weights[k]
                inverse = 1.0 / target
                rows = pl.ds(lon0 * LEV + k, count, stride=LEV)
                thick_ref[rows, :] = (target * self.scale)[0:count, 0:96]
                temp_ref[rows, :] = ((temps[n] - previous[0]) * inverse)[0:count, 0:96]
                tracer_ref[rows, :] = ((tracs[n] - previous[1]) * inverse)[0:count, 0:96]
                previous = (temps[n], tracs[n])


def on_device(th, te, tr, ec, nc, polar_mask, wave_cutoff, level_weight, target_surface):
    vmem = pl.BlockSpec(memory_space=pltpu.VMEM)
    hbm = pl.BlockSpec(memory_space=pl.ANY)
    full, real = tables()
    dma = pltpu.SemaphoreType.DMA
    chunks = len(CHUNKS)
    fields = tuple(jax.ShapeDtypeStruct((36 * LEV, 96), F32) for _ in range(3))
    late = jax.ShapeDtypeStruct((NLEVD, NX, 16, 128), F32)
    quarter = jax.ShapeDtypeStruct((NLEVD, NX, 8, 128), F32)
    scale = jax.ShapeDtypeStruct((8, 128), F32)
    parts = pl.pallas_call(
        step_kernel,
        name="step",
        out_shape=fields + (late, quarter, scale),
        in_specs=[hbm] * 11,
        out_specs=(hbm,) * 6,
        scratch_shapes=[pltpu.VMEM(o.shape, F32) for o in fields + (scale,)]
        + [
            pltpu.VMEM((5, LEVD, ROWS, NLON), F32),
            pltpu.VMEM(full.shape, BF16),
            pltpu.VMEM(real.shape, BF16),
            pltpu.VMEM((3, LEVD, ROWS, NLON), F32),
            pltpu.VMEM((16, NLON), F32),
            pltpu.VMEM((12, NLON), F32),
            pltpu.VMEM((16, NLON), F32),
            pltpu.VMEM((12, NLON), F32),
            pltpu.VMEM((32, NLON), F32),
            pltpu.VMEM((288, NLON), BF16),
            pltpu.VMEM((288, NLON), BF16),
            pltpu.VMEM((288, NLON), F32),
            pltpu.VMEM((3, NLON, 128), F32),
            pltpu.VMEM((NLATD, SENT, 128), F32),
            pltpu.VMEM((NLATD, SENT, 128), F32),
            pltpu.VMEM((NLEVD, NX, SENT, 128), F32),
            pltpu.VMEM((1, 128), F32),
            pltpu.VMEM((NZ, 1, 128), F32),
            pltpu.VMEM((NX * NLEVD, NZ, 1, 128), F32),
            pltpu.VMEM((3, LEV, 40, 128), F32),
            dma((11,)), dma((2,)), dma((2,)), dma((1,)),
            dma((chunks,)), dma((chunks, NZ)), dma((1,)), dma((1,)), dma((1,)), dma((1,)),
            dma((chunks,)), dma((chunks,)),
            pltpu.SMEM((ROWS,), jnp.int32), pltpu.SMEM((ROWS,), jnp.int32),
            pltpu.SMEM((LEV,), F32), pltpu.SMEM((1,), F32), dma((5,)),
        ],
        compiler_params=pltpu.CompilerParams(
            collective_id=0, has_side_effects=True, vmem_limit_bytes=67043328
        ),
    )(th, te, tr, ec, nc, polar_mask, wave_cutoff, level_weight, target_surface, jnp.asarray(full), jnp.asarray(real))
    outs = pl.pallas_call(
        finish_kernel,
        name="finish",
        out_shape=fields,
        in_specs=[hbm] * 7,
        out_specs=(vmem,) * 3,
        scratch_shapes=[
            pltpu.VMEM(late.shape, F32), pltpu.VMEM(quarter.shape, F32), pltpu.VMEM(scale.shape, F32),
            pltpu.VMEM((3, LEV, 8, 128), F32), pltpu.SMEM((LEV,), F32), dma((7,)),
        ],
        compiler_params=pltpu.CompilerParams(vmem_limit_bytes=67043328),
    )(*parts, level_weight)
    return tuple(o.reshape(36, LEV, 96).transpose(1, 2, 0) for o in outs)


def solution(mesh):
    field = P("lev", "lat", None)
    return jax.shard_map(
        on_device,
        mesh=mesh,
        in_specs=(field,) * 5 + (P("lat"), P("lat"), P(), P()),
        out_specs=(P(None, "lev", "lat"),) * 3,
        check_vma=False,
    )
```

```python
import functools

import jax
import jax.numpy as jnp
import numpy as np
from jax import lax
from jax.experimental import pallas as pl
from jax.experimental.pallas import tpu as pltpu
from jax.sharding import PartitionSpec as P

MESH = pl.DeviceIdType.MESH
F32 = jnp.float32
BF16 = jnp.bfloat16

NLON, NLAT, LEV = 1152, 768, 32
ROWS = 24
LEVD = 4
NZ, NX, NY = 8, 4, 4
NLATD, NLEVD = 32, 8
RADIX, POINTS = 9, 128
SENT = 84
POLAR_BANDS = -(-(NLAT // 5) // ROWS)


def split_bf16(x):
    high = x.astype(BF16)
    return high, (x - high.astype(F32)).astype(BF16)


def tables():
    b = np.arange(POINTS)[:, None]
    full = np.zeros((4, 256, 256))
    for k1 in range(1, 5):
        angle = 2.0 * np.pi * ((b * (k1 + RADIX * np.arange(POINTS)[None, :])) % NLON) / NLON
        c, s = np.cos(angle), np.sin(angle)
        full[k1 - 1] = np.block([[c, -s], [s, c]])
    col = np.arange(POINTS)[None, :]
    wave = np.where(col <= 64, col, col - 64)
    angle = 2.0 * np.pi * ((b * wave) % POINTS) / POINTS
    real = np.where(col <= 64, np.cos(angle), np.sin(angle))

    def pair(x):
        high = x.astype(np.float32).astype(BF16)
        low = (x - high.astype(np.float64)).astype(np.float32).astype(BF16)
        return np.stack([np.asarray(high), np.asarray(low)])

    return pair(full), pair(real)


def dot3(xh, xl, th, tl, dims):
    dot = functools.partial(
        lax.dot_general, dimension_numbers=(dims, ((), ())), preferred_element_type=F32
    )
    rows = xh.shape[0]
    both = dot(jnp.concatenate([xh, xl], axis=0), th)
    return both[:rows] + both[rows:] + dot(xh, tl)


def lanes9(x):
    return jnp.concatenate([x] * RADIX, axis=1)


def step_kernel(
    th_hbm, te_hbm, tr_hbm, ec_hbm, nc_hbm, mask_hbm, cut_hbm, weight_hbm, target_hbm, full_hbm, real_hbm,
    thick_hbm, temp_hbm, tracer_hbm, late_hbm, quarter_hbm, scale_hbm,
    thick_ref, temp_ref, tracer_ref, scale_ref,
    in_ref, full_ref, real_ref, s_ref, up_ref, down_ref, from_south, from_north, edge_ref, uh_ref, ul_ref, z_ref, t_ref,
    msg_ref, mid_ref, col_ref, part_ref, ring_sum, all_sum, r_ref,
    load_sem, halo_send, halo_recv, own_sem, zs, zr, ps, pr, rs, rr, fs, fr,
    mask_ref, cut_ref, weight_ref, target_ref, out_sem,
):
    lat = lax.axis_index("lat")
    lev = lax.axis_index("lev")
    z, x = lat // NX, lax.rem(lat, NX)
    north = lax.rem(lat + 1, NLATD)
    south = lax.rem(lat + NLATD - 1, NLATD)
    polar = jnp.logical_or(lat < POLAR_BANDS, lat >= NLATD - POLAR_BANDS)

    fields_hbm = (th_hbm, te_hbm, tr_hbm, nc_hbm, ec_hbm)
    loads = [pltpu.make_async_copy(fields_hbm[f], in_ref.at[f], load_sem.at[f]) for f in range(5)]
    small = ((mask_hbm, mask_ref), (cut_hbm, cut_ref), (weight_hbm, weight_ref), (target_hbm, target_ref))
    loads += [pltpu.make_async_copy(a, b, load_sem.at[7 + n]) for n, (a, b) in enumerate(small)]
    for load in loads:
        load.start()
    barrier = pltpu.get_barrier_semaphore()
    for other in (north, south):
        pl.semaphore_signal(barrier, inc=1, device_id=(other, lev), device_id_type=MESH)

    def plane_peer(o):
        return z * NX + lax.rem(x + o // NLEVD, NX), lax.rem(lev + o, NLEVD)

    def greet_plane(o, carry):
        pl.semaphore_signal(barrier, inc=1, device_id=plane_peer(o), device_id_type=MESH)
        return carry

    def greet_ring(o, carry):
        peer = (lax.rem(lat + NX * o, NLATD), lev)
        pl.semaphore_signal(barrier, inc=1, device_id=peer, device_id_type=MESH)
        return carry

    lax.fori_loop(1, NZ, greet_ring, 0)
    lax.fori_loop(1, NX * NLEVD, greet_plane, 0)

    table_loads = (
        pltpu.make_async_copy(full_hbm, full_ref, load_sem.at[5]),
        pltpu.make_async_copy(real_hbm, real_ref, load_sem.at[6]),
    )

    @pl.when(polar)
    def _():
        for load in table_loads:
            load.start()

    for load in loads:
        load.wait()
    th_ref, te_ref, tr_ref, nc_ref, ec_ref = (in_ref.at[f] for f in range(5))
    fields = (th_ref, te_ref, tr_ref, nc_ref)
    for f in range(4):
        for l in range(LEVD):
            up_ref[pl.ds(4 * f + l, 1), :] = fields[f][l, ROWS - 1 : ROWS, :]
            if f < 3:
                down_ref[pl.ds(4 * f + l, 1), :] = fields[f][l, 0:1, :]

    def east(l, carry):
        th, te, tr = th_ref[l], te_ref[l], tr_ref[l]
        mass = ec_ref[l] * (th + pltpu.roll(th, NLON - 1, 1)) * 0.5
        temp = mass * (te + pltpu.roll(te, NLON - 1, 1)) * 0.5
        trac = mass * (tr + pltpu.roll(tr, NLON - 1, 1)) * 0.5
        s_ref[0, l] = pltpu.roll(mass, 1, 1) - mass
        s_ref[1, l] = pltpu.roll(temp, 1, 1) - temp
        s_ref[2, l] = pltpu.roll(trac, 1, 1) - trac
        return carry

    lax.fori_loop(0, LEVD, east, 0)

    first_row = lat * ROWS
    row = (first_row + lax.broadcasted_iota(jnp.int32, (ROWS, 128), 0)).astype(F32)
    center = lanes9(jnp.sin((row + 0.5) * np.float32(np.pi) / NLAT))
    face = lanes9(jnp.sin((row + 1.0) * np.float32(np.pi) / NLAT))
    inverse_center = 1.0 / center
    row_in = lax.broadcasted_iota(jnp.int32, (ROWS, NLON), 0)

    def inner(l, carry):
        th, te, tr = th_ref[l], te_ref[l], tr_ref[l]

        def above(v):
            return pltpu.roll(v, ROWS - 1, 0)

        mass = nc_ref[l] * (th + above(th)) * 0.5 * face
        mass = jnp.where(row_in == ROWS - 1, 0.0, mass)
        temp = mass * (te + above(te)) * 0.5
        trac = mass * (tr + above(tr)) * 0.5
        for f, flux in enumerate((mass, temp, trac)):
            s_ref[f, l] = s_ref[f, l] - (flux - pltpu.roll(flux, 1, 0)) * inverse_center
        return carry

    lax.fori_loop(0, LEVD, inner, 0)
    flat = s_ref.reshape(3 * LEVD * ROWS, NLON)
    scratch = full_ref, real_ref, uh_ref, ul_ref, z_ref

    @pl.when(polar)
    def _():
        for load in table_loads:
            load.wait()
        cuts = row_cuts(mask_ref, cut_ref)
        polar_filter(flat, 3 * LEVD * ROWS, jnp.concatenate([cuts] * (3 * LEVD), axis=0), *scratch)

    pl.semaphore_wait(barrier, 2 + NZ - 1 + NX * NLEVD - 1)
    to_north = pltpu.make_async_remote_copy(
        src_ref=up_ref, dst_ref=from_south, send_sem=halo_send.at[0], recv_sem=halo_recv.at[0],
        device_id=(north, lev), device_id_type=MESH,
    )
    to_south = pltpu.make_async_remote_copy(
        src_ref=down_ref, dst_ref=from_north, send_sem=halo_send.at[1], recv_sem=halo_recv.at[1],
        device_id=(south, lev), device_id_type=MESH,
    )
    has_north, has_south = lat < NLATD - 1, lat > 0
    pl.when(has_north)(to_north.start)
    pl.when(has_south)(to_south.start)
    pl.when(has_south)(to_north.wait_recv)
    pl.when(has_north)(to_south.wait_recv)

    def rows_of(ref, f):
        return ref[4 * f : 4 * f + 4, :]

    def beyond(ref, f, there):
        return jnp.where(there, rows_of(ref, f), 0.0)

    def faces(courant, own, other, face_row):
        mass = courant * (own[0] + other[0]) * 0.5 * face_row
        return mass, mass * (own[1] + other[1]) * 0.5, mass * (own[2] + other[2]) * 0.5

    top = faces(
        rows_of(up_ref, 3), [rows_of(up_ref, f) for f in range(3)],
        [beyond(from_north, f, has_north) for f in range(3)], face[ROWS - 1 : ROWS],
    )
    bottom = faces(
        beyond(from_south, 3, has_south), [beyond(from_south, f, has_south) for f in range(3)],
        [rows_of(down_ref, f) for f in range(3)], face_below_row(first_row),
    )
    for f in range(3):
        edge_ref[4 * f : 4 * f + 4, :] = -top[f] * inverse_center[ROWS - 1 : ROWS]
        edge_ref[12 + 4 * f : 16 + 4 * f, :] = bottom[f] * inverse_center[0:1]
    edge_ref[24:32, :] = jnp.zeros((8, NLON), F32)

    @pl.when(polar)
    def _():
        cuts = row_cuts(mask_ref, cut_ref)
        edge_row = lax.broadcasted_iota(jnp.int32, (32, 128), 0)
        cuts = jnp.where(edge_row < 12, cuts[ROWS - 1 : ROWS], cuts[0:1])
        polar_filter(edge_ref, 32, cuts, *scratch)

    for f in range(3):
        for l in range(LEVD):
            n = 4 * f + l
            s_ref[f, l, ROWS - 1 : ROWS, :] = s_ref[f, l, ROWS - 1 : ROWS, :] + edge_ref[n : n + 1, :]
            s_ref[f, l, 0:1, :] = s_ref[f, l, 0:1, :] + edge_ref[12 + n : 13 + n, :]
    pl.when(has_north)(to_north.wait_send)
    pl.when(has_south)(to_south.wait_send)

    def update(l, total):
        th, te, tr = th_ref[l], te_ref[l], tr_ref[l]
        mass = s_ref[0, l]
        inverse = 1.0 / th
        new_th = th + mass
        s_ref[0, l] = new_th
        s_ref[1, l] = te + (s_ref[1, l] - te * mass) * inverse
        s_ref[2, l] = tr + (s_ref[2, l] - tr * mass) * inverse
        weighted = new_th * center
        for a in range(RADIX):
            part = weighted[:, 128 * a : 128 * a + 128]
            total = total + (part[0:8] + part[8:16] + part[16:24])
        return total

    total = lax.fori_loop(0, LEVD, update, jnp.zeros((8, 128), F32))
    total = jnp.sum(total, axis=0, keepdims=True)
    part_ref[...] = total
    ring_sum[z] = total

    for a in range(RADIX):
        at = pl.ds(128 * a, 128)
        one = jnp.concatenate([flat[0:120, at], flat[264:272, at]], axis=0)
        two = jnp.concatenate([flat[120:240, at], flat[272:280, at]], axis=0)
        last = jnp.concatenate([flat[240:264, at], flat[280:288, at]], axis=0)
        t_ref[0, at, :] = one.T
        t_ref[1, at, :] = two.T
        t_ref[2, at, :] = jnp.concatenate([last] * 4, axis=0).T

    sub = lax.broadcasted_iota(jnp.int32, (8, 128), 0)
    lane = lax.broadcasted_iota(jnp.int32, (8, 128), 1)

    def pack(p, carry):
        base = 72 * p

        def tile(q, j, n=1):
            return t_ref[q, pl.ds(pl.multiple_of(base + 8 * j, 8), 8 * n), :]

        def fours(u):
            return jnp.where(
                lane < 64, jnp.where(lane < 32, u[0], u[1]), jnp.where(lane < 96, u[2], u[3])
            )

        for q in range(2):
            for j in range(4):
                at = pl.ds(TILE_ROW[j] + TILE_STEP[j] * q, 8)
                msg_ref[2 * p, at, :] = tile(q, j)
                msg_ref[2 * p + 1, at, :] = tile(q, 5 + j)
        t0, t1, t2 = tile(0, 4), tile(1, 4), tile(2, 4)
        msg_ref[2 * p, 72:80, :] = jnp.where(sub < 4, t0, pltpu.roll(t1, 4, 0))
        msg_ref[2 * p + 1, 72:80, :] = jnp.where(sub < 4, pltpu.roll(t0, 4, 0), t1)
        msg_ref[2 * p, 32:40, :] = fours([tile(2, j) for j in range(4)])
        msg_ref[2 * p + 1, 32:40, :] = fours([tile(2, j) for j in range(5, 9)])
        msg_ref[2 * p, 80:84, :] = t2[0:4]
        msg_ref[2 * p + 1, 80:84, :] = pltpu.roll(t2, 4, 0)[0:4]
        return carry

    lax.fori_loop(0, NLATD // 2, pack, 0)

    def ring_part(o):
        return pltpu.make_async_remote_copy(
            src_ref=part_ref, dst_ref=ring_sum.at[z], send_sem=ps.at[0], recv_sem=pr.at[0],
            device_id=(lax.rem(lat + NX * o, NLATD), lev), device_id_type=MESH,
        )

    def plane_part(o):
        return pltpu.make_async_remote_copy(
            src_ref=ring_sum, dst_ref=all_sum.at[x * NLEVD + lev], send_sem=rs.at[0], recv_sem=rr.at[0],
            device_id=plane_peer(o), device_id_type=MESH,
        )

    def all_of(ref, sem):
        pltpu.make_async_copy(ref, ref, sem).wait()

    def each(count, action, start=0):
        def body(o, carry):
            action(o)
            return carry

        lax.fori_loop(start, count, body, 0)

    each(NZ, lambda o: ring_part(o).start(), 1)

    def distance(k):
        ahead = jnp.where(lax.rem(k, 2) == 1, (k + 1) // 2, lax.rem(NZ - k // 2, NZ))
        return jnp.where(lax.rem(lev // 2, 2) == 0, ahead, lax.rem(NZ - ahead, NZ))

    def along_z(chunk, k):
        to = lax.rem(z + distance(k), NZ)
        first, count = CHUNKS[chunk]
        return pltpu.make_async_remote_copy(
            src_ref=msg_ref.at[pl.ds(NX * to, NX), pl.ds(first, count)],
            dst_ref=mid_ref.at[pl.ds(NX * z, NX), pl.ds(first, count)],
            send_sem=zs.at[chunk], recv_sem=zr.at[chunk, k],
            device_id=(to * NX + x, lev), device_id_type=MESH,
        )

    for chunk in range(len(CHUNKS)):
        each(NZ, lambda k: along_z(chunk, k).start(), 1)
    mine = pltpu.make_async_copy(
        msg_ref.at[pl.ds(NX * z, NX)], mid_ref.at[pl.ds(NX * z, NX)], own_sem.at[0]
    )
    mine.start()

    mine.wait()

    def onward(chunk, source, to_x):
        first, count = CHUNKS[chunk]
        piece = mid_ref.at[NX * source + to_x, pl.ds(first, count)]
        place = late_hbm.at[lev, x] if chunk == LAST else col_ref.at[lev, x, pl.ds(first, count)]
        away = pltpu.make_async_remote_copy(
            src_ref=piece, dst_ref=place, send_sem=fs.at[chunk], recv_sem=fr.at[chunk],
            device_id=(z * NX + to_x, source), device_id_type=MESH,
        )
        stay = pltpu.make_async_copy(piece, place, fr.at[chunk])
        return away, stay

    def forward(chunk, k):
        source = lax.rem(z + NZ - distance(k), NZ)

        @pl.when(k > 0)
        def _():
            along_z(chunk, k).wait_recv()

        for dx in ACROSS:
            away, stay = onward(chunk, source, lax.rem(x + dx, NX))
            if dx == 0:
                pl.when(source != lev)(away.start)
                pl.when(source == lev)(stay.start)
            else:
                away.start()

    def arrived(chunk):
        first, count = CHUNKS[chunk]
        all_of(mid_ref.at[:, pl.ds(first, count)], fr.at[chunk])

    remap = Remap(lat, lane, r_ref, weight_ref, thick_ref, temp_ref, tracer_ref)

    each(1, lambda k: forward(0, k))
    all_of(ring_sum.at[pl.ds(0, NZ - 1)], pr.at[0])
    each(NX * NLEVD, lambda o: plane_part(o).start(), 1)
    each(NZ, lambda k: forward(0, k), 1)
    each(NZ, lambda k: forward(1, k))
    all_of(all_sum.at[pl.ds(0, NX * NLEVD - 1)], rr.at[0])
    all_sum[x * NLEVD + lev] = ring_sum[...]
    scale_ref[...] = mass_scale(all_sum, target_ref)
    remap.scale = scale_ref[...]
    arrived(0)
    quarter = pltpu.make_async_copy(col_ref.at[:, :, pl.ds(32, 8)], quarter_hbm, out_sem.at[4])
    quarter.start()
    remap.unpack(from_columns(col_ref, 0))
    remap.tile(0)
    each(3, lambda k: forward(2, k))
    remap.unpack(from_columns(col_ref, 1))
    remap.tile(1)
    each(NZ, lambda k: forward(2, k), 3)
    arrived(1)
    remap.unpack(from_columns(col_ref, 2))
    remap.tile(2)
    remap.unpack(from_columns(col_ref, 4))
    remap.half_tile()
    outs = ((thick_ref, thick_hbm), (temp_ref, temp_hbm), (tracer_ref, tracer_hbm), (scale_ref, scale_hbm))
    stores = [pltpu.make_async_copy(a, b, out_sem.at[n]) for n, (a, b) in enumerate(outs)]
    for store in stores:
        store.start()
    all_of(ring_sum.at[pl.ds(0, NZ - 1)], ps.at[0])
    all_of(all_sum.at[pl.ds(0, NX * NLEVD - 1)], rs.at[0])
    for chunk, (first, count) in enumerate(CHUNKS):
        all_of(mid_ref.at[pl.ds(0, NX * (NZ - 1)), pl.ds(first, count)], zs.at[chunk])
        all_of(mid_ref.at[pl.ds(0, NX * NLEVD - 1), pl.ds(first, count)], fs.at[chunk])
    quarter.wait()
    for store in stores:
        store.wait()
    arrived(LAST)


def finish_kernel(
    thick_hbm, temp_hbm, tracer_hbm, late_hbm, quarter_hbm, scale_hbm, weight_hbm,
    thick_ref, temp_ref, tracer_ref,
    late_ref, quarter_ref, scale_ref, r_ref, weight_ref, sem,
):
    lat = lax.axis_index("lat")
    pairs = (
        (late_hbm, late_ref), (quarter_hbm, quarter_ref), (scale_hbm, scale_ref), (weight_hbm, weight_ref),
        (thick_hbm, thick_ref), (temp_hbm, temp_ref), (tracer_hbm, tracer_ref),
    )
    loads = [pltpu.make_async_copy(a, b, sem.at[n]) for n, (a, b) in enumerate(pairs)]
    for load in loads:
        load.start()
    for load in loads[:4]:
        load.wait()
    lane = lax.broadcasted_iota(jnp.int32, (8, 128), 1)
    remap = Remap(lat, lane, r_ref, weight_ref, thick_ref, temp_ref, tracer_ref)
    remap.scale = scale_ref[...]

    def pieces(g):
        one = [late_ref[g, x, 0:8, :] for x in range(4)]
        two = [late_ref[g, x, 8:16, :] for x in range(4)]
        return one, two, [quarter_ref[g, x] for x in range(4)], 96

    remap.unpack((0, pieces))
    for load in loads[4:]:
        load.wait()
    remap.columns(0, 8, 24 + 4 * remap.odd)


def face_below_row(first_row):
    row = lax.broadcasted_iota(jnp.int32, (8, 128), 0) * 0 + first_row
    below = jnp.sin(row.astype(F32) * np.float32(np.pi) / NLAT)
    return lanes9(below[0:1])


def row_cuts(mask_ref, cut_ref):
    row = lax.broadcasted_iota(jnp.int32, (ROWS, 128), 0)
    cuts = jnp.full((ROWS, 128), NLON, jnp.int32)
    for r in range(ROWS):
        cuts = jnp.where(row == r, jnp.where(mask_ref[r] > 0, cut_ref[r], NLON), cuts)
    return cuts


def polar_filter(flat, rows, cuts, full_ref, real_ref, uh_ref, ul_ref, z_ref):
    cos9 = [[np.float32(np.cos(2 * np.pi * a * k / 9)) for k in range(5)] for a in range(5)]
    sin9 = [[np.float32(np.sin(2 * np.pi * a * k / 9)) for k in range(5)] for a in range(5)]

    def forward(r, carry):
        at = pl.ds(pl.multiple_of(16 * r, 16), 16)
        v = [flat[at, 128 * a : 128 * a + 128] for a in range(RADIX)]
        even = [v[a] + v[9 - a] for a in range(1, 5)]
        odd = [v[a] - v[9 - a] for a in range(1, 5)]

        def put(slot, x):
            high, low = split_bf16(x)
            uh_ref[at, 128 * slot : 128 * slot + 128] = high
            ul_ref[at, 128 * slot : 128 * slot + 128] = low

        put(8, v[0] + ((even[0] + even[1]) + (even[2] + even[3])))
        for k in range(1, 5):
            put(2 * k - 2, v[0] + sum(even[a - 1] * cos9[a][k] for a in range(1, 5)))
            put(2 * k - 1, -sum(odd[a - 1] * sin9[a][k] for a in range(1, 5)))
        return carry

    lax.fori_loop(0, rows // 16, forward, 0)

    lane = lax.broadcasted_iota(jnp.int32, (rows, 128), 1)
    here = pl.ds(0, rows)
    for k in range(1, 5):
        wave = k + RADIX * lane
        keep = (jnp.minimum(wave, NLON - wave) >= cuts).astype(F32)
        keep = jnp.concatenate([keep, keep], axis=1)
        at = pl.ds(256 * (k - 1), 256)
        tables_k = full_ref[0, k - 1], full_ref[1, k - 1]
        x = dot3(uh_ref[here, at], ul_ref[here, at], *tables_k, ((1,), (0,)))
        xh, xl = split_bf16(x * keep)
        z_ref[here, at] = dot3(xh, xl, *tables_k, ((1,), (1,)))
    at = pl.ds(1024, 128)
    wave = RADIX * jnp.where(lane <= 64, lane, lane - 64)
    weight = jnp.where(jnp.logical_or(lane == 0, lane == 64), 1.0, 2.0)
    keep = jnp.where(wave >= cuts, weight, 0.0)
    x = dot3(uh_ref[here, at], ul_ref[here, at], real_ref[0], real_ref[1], ((1,), (0,)))
    xh, xl = split_bf16(x * keep)
    z_ref[here, at] = dot3(xh, xl, real_ref[0], real_ref[1], ((1,), (1,)))

    def backward(r, carry):
        at = pl.ds(pl.multiple_of(8 * r, 8), 8)
        z0 = z_ref[at, 1024:1152] * np.float32(1.0 / NLON)
        zr = [z_ref[at, 256 * k : 256 * k + 128] * np.float32(2.0 / NLON) for k in range(4)]
        zi = [z_ref[at, 256 * k + 128 : 256 * k + 256] * np.float32(2.0 / NLON) for k in range(4)]
        flat[at, 0:128] = flat[at, 0:128] - (z0 + ((zr[0] + zr[1]) + (zr[2] + zr[3])))
        for a in range(1, 5):
            even = z0 + sum(zr[k - 1] * cos9[a][k] for k in range(1, 5))
            odd = sum(zi[k - 1] * sin9[a][k] for k in range(1, 5))
            lo, hi = pl.ds(128 * a, 128), pl.ds(128 * (9 - a), 128)
            flat[at, lo] = flat[at, lo] - (even - odd)
            flat[at, hi] = flat[at, hi] - (even + odd)
        return carry

    lax.fori_loop(0, rows // 8, backward, 0)


ACROSS = (0, 1, 3, 2)
CHUNKS = ((0, 40), (56, 28), (40, 16))
TILE_ROW = (0, 8, 56, 40)
TILE_STEP = (16, 16, 8, 8)


LAST = 2


def mass_scale(all_sum, target_ref):
    area = float(np.sum(np.sin((np.arange(NLAT) + 0.5) * np.pi / NLAT)))
    total = jnp.sum(all_sum[...].reshape(NX * NLEVD * NZ, 128), axis=0, keepdims=True)
    total = jnp.sum(total, axis=1, keepdims=True)
    return jnp.broadcast_to(target_ref[0] * (NLON * area) / total, (8, 128))


def from_columns(col_ref, j):
    def pieces(g):
        if j < 4:
            one = [col_ref[g, x, pl.ds(TILE_ROW[j], 8), :] for x in range(4)]
            two = [col_ref[g, x, pl.ds(TILE_ROW[j] + TILE_STEP[j], 8), :] for x in range(4)]
            return one, two, [col_ref[g, x, 32:40, :] for x in range(4)], 32 * j
        one = [col_ref[g, x, 72:80, :] for x in range(4)]
        two = [pltpu.roll(v, 4, 0) for v in one]
        last = [col_ref[g, x, 80:84, :] for x in range(4)]
        return one, two, [jnp.concatenate([v, v], axis=0) for v in last], 0

    return j, pieces


class Remap:
    def __init__(self, lat, lane, r_ref, weight_ref, thick_ref, temp_ref, tracer_ref):
        self.odd = lax.rem(lat, 2)
        self.lane = lane
        self.r_ref = r_ref
        self.outs = thick_ref, temp_ref, tracer_ref
        self.weights = [weight_ref[k] for k in range(LEV)]
        whole = self.weights[0]
        for k in range(1, LEV):
            whole = whole + self.weights[k]
        self.whole = whole

    def unpack(self, tile):
        lane, r_ref = self.lane, self.r_ref
        j, pieces = tile

        def merge(parts):
            return jnp.where(
                lane < 48, jnp.where(lane < 24, parts[0], parts[1]), jnp.where(lane < 72, parts[2], parts[3])
            )

        def move(v, source, target):
            amount = (target - source) % 128
            return v if amount == 0 else pltpu.roll(v, amount, 1)

        phase = jnp.where(
            lane >= 72, lane - 72, jnp.where(lane >= 48, lane - 48, jnp.where(lane >= 24, lane - 24, lane))
        )

        def body(g, carry):
            one, two, last, lane0 = pieces(g)

            def put(fl, v):
                r_ref[fl // 4, g * 4 + fl % 4, 8 * j : 8 * j + 8, :] = v

            for n in range(5):
                put(n, merge([move(one[x], 24 * n, 24 * x) for x in range(4)]))
                put(5 + n, merge([move(two[x], 24 * n, 24 * x) for x in range(4)]))
            put(10, merge([move(last[x], lane0, 24 * x) for x in range(4)]))
            a = merge([move(one[x], 120, 24 * x) for x in range(4)])
            b = merge([move(two[x], 120, 24 * x + 8) for x in range(4)])
            c = merge([move(last[x], lane0 + 24, 24 * x + 16) for x in range(4)])
            put(11, jnp.where(phase < 8, a, jnp.where(phase < 16, b, c)))
            return carry

        lax.fori_loop(0, NLEVD, body, 0)

    def tile(self, j):
        self.columns(j, 8, 8 * j + 4 * self.odd)

    def half_tile(self):
        self.columns(4, 4, 32 - 32 * self.odd)

    def columns(self, j, count, lon0):
        weights, r_ref = self.weights, self.r_ref
        thick_ref, temp_ref, tracer_ref = self.outs
        at = pl.ds(pl.multiple_of(8 * j, 8), 8)
        surface = r_ref[0, 0, at, :]
        for m in range(1, LEV):
            surface = surface + r_ref[0, m, at, :]
        unit = surface / jnp.full((8, 128), self.whole)
        previous = (jnp.zeros((8, 128), F32), jnp.zeros((8, 128), F32))
        running = None
        for k0 in range(0, LEV, 8):
            bounds = []
            for k in range(k0, k0 + 8):
                running = weights[k] if running is None else running + weights[k]
                bounds.append(unit * running)
            temps = [jnp.zeros((8, 128), F32)] * 8
            tracs = [jnp.zeros((8, 128), F32)] * 8
            top = jnp.zeros((8, 128), F32)
            for m in range(LEV):
                th = r_ref[0, m, at, :]
                te = r_ref[1, m, at, :]
                tr = r_ref[2, m, at, :]
                for n in range(8):
                    part = jnp.minimum(jnp.maximum(bounds[n] - top, 0.0), th)
                    temps[n] = temps[n] + te * part
                    tracs[n] = tracs[n] + tr * part
                top = top + th
            for n in range(8):
                k = k0 + n
                target = unit * weights[k]
                inverse = 1.0 / target
                rows = pl.ds(lon0 * LEV + k, count, stride=LEV)
                thick_ref[rows, :] = (target * self.scale)[0:count, 0:96]
                temp_ref[rows, :] = ((temps[n] - previous[0]) * inverse)[0:count, 0:96]
                tracer_ref[rows, :] = ((tracs[n] - previous[1]) * inverse)[0:count, 0:96]
                previous = (temps[n], tracs[n])


def on_device(th, te, tr, ec, nc, polar_mask, wave_cutoff, level_weight, target_surface):
    vmem = pl.BlockSpec(memory_space=pltpu.VMEM)
    hbm = pl.BlockSpec(memory_space=pl.ANY)
    full, real = tables()
    dma = pltpu.SemaphoreType.DMA
    chunks = len(CHUNKS)
    fields = tuple(jax.ShapeDtypeStruct((36 * LEV, 96), F32) for _ in range(3))
    late = jax.ShapeDtypeStruct((NLEVD, NX, 16, 128), F32)
    quarter = jax.ShapeDtypeStruct((NLEVD, NX, 8, 128), F32)
    scale = jax.ShapeDtypeStruct((8, 128), F32)
    parts = pl.pallas_call(
        step_kernel,
        name="step",
        out_shape=fields + (late, quarter, scale),
        in_specs=[hbm] * 11,
        out_specs=(hbm,) * 6,
        scratch_shapes=[pltpu.VMEM(o.shape, F32) for o in fields + (scale,)]
        + [
            pltpu.VMEM((5, LEVD, ROWS, NLON), F32),
            pltpu.VMEM(full.shape, BF16),
            pltpu.VMEM(real.shape, BF16),
            pltpu.VMEM((3, LEVD, ROWS, NLON), F32),
            pltpu.VMEM((16, NLON), F32),
            pltpu.VMEM((12, NLON), F32),
            pltpu.VMEM((16, NLON), F32),
            pltpu.VMEM((12, NLON), F32),
            pltpu.VMEM((32, NLON), F32),
            pltpu.VMEM((288, NLON), BF16),
            pltpu.VMEM((288, NLON), BF16),
            pltpu.VMEM((288, NLON), F32),
            pltpu.VMEM((3, NLON, 128), F32),
            pltpu.VMEM((NLATD, SENT, 128), F32),
            pltpu.VMEM((NLATD, SENT, 128), F32),
            pltpu.VMEM((NLEVD, NX, SENT, 128), F32),
            pltpu.VMEM((1, 128), F32),
            pltpu.VMEM((NZ, 1, 128), F32),
            pltpu.VMEM((NX * NLEVD, NZ, 1, 128), F32),
            pltpu.VMEM((3, LEV, 40, 128), F32),
            dma((11,)), dma((2,)), dma((2,)), dma((1,)),
            dma((chunks,)), dma((chunks, NZ)), dma((1,)), dma((1,)), dma((1,)), dma((1,)),
            dma((chunks,)), dma((chunks,)),
            pltpu.SMEM((ROWS,), jnp.int32), pltpu.SMEM((ROWS,), jnp.int32),
            pltpu.SMEM((LEV,), F32), pltpu.SMEM((1,), F32), dma((5,)),
        ],
        compiler_params=pltpu.CompilerParams(
            collective_id=0, has_side_effects=True, vmem_limit_bytes=67043328
        ),
    )(th, te, tr, ec, nc, polar_mask, wave_cutoff, level_weight, target_surface, jnp.asarray(full), jnp.asarray(real))
    outs = pl.pallas_call(
        finish_kernel,
        name="finish",
        out_shape=fields,
        in_specs=[hbm] * 7,
        out_specs=(vmem,) * 3,
        scratch_shapes=[
            pltpu.VMEM(late.shape, F32), pltpu.VMEM(quarter.shape, F32), pltpu.VMEM(scale.shape, F32),
            pltpu.VMEM((3, LEV, 8, 128), F32), pltpu.SMEM((LEV,), F32), dma((7,)),
        ],
        compiler_params=pltpu.CompilerParams(vmem_limit_bytes=67043328),
    )(*parts, level_weight)
    return tuple(o.reshape(36, LEV, 96).transpose(1, 2, 0) for o in outs)


def solution(mesh):
    field = P("lev", "lat", None)
    return jax.shard_map(
        on_device,
        mesh=mesh,
        in_specs=(field,) * 5 + (P("lat"), P("lat"), P(), P()),
        out_specs=(P(None, "lev", "lat"),) * 3,
        check_vma=False,
    )
```
